32 devices in a mesh: row: 16 (over z, x, core), ch: 2 (over y).
Axes of the slice: x: 2, y: 2, z: 4, core: 2. Of those that a mesh axis runs over, the one named last changes fastest.
Arguments:
- pair_rep: float32 [256, 256, 128], P('row', 'ch'), may hold values from -6 to 6
- residue_mask: int32 [256], replicated, may hold values 0 or 1
- pair_gain: float32 [2, 128], replicated, may hold values from 0.5 to 1.5
- pair_shift: float32 [2, 128], replicated, may hold values from -3 to 3
- panel_weight: bfloat16 [2, 128, 512], replicated, may hold values from -0.5 to 0.5
- panel_bias: float32 [2, 512], replicated, may hold values from -3 to 3
- gate_weight: bfloat16 [2, 128, 128], replicated, may hold values from -0.5 to 0.5
- gate_bias: float32 [2, 128], replicated, may hold values from -3 to 3
- hidden_gain: float32 [2, 128], replicated, may hold values from 0.5 to 1.5
- hidden_shift: float32 [2, 128], replicated, may hold values from -3 to 3
- output_weight: bfloat16 [2, 128, 128], replicated, may hold values from -0.5 to 0.5
- output_bias: float32 [2, 128], replicated, may hold values from -3 to 3
Outputs:
- updated_pair: float32 [256, 256, 128], P('row', 'ch')
The draws below stay inside these ranges and needn't reach their ends.
All inputs are finite; a program needn't handle non-finite values.
Results may differ from the reference program's by a relative error of at most 0.0039.
Values may be sent and summed in bfloat16 or wider, within the bound.
A program may use at most 64 MiB of HBM per device.

```python
import math
import jax
import jax.numpy as jnp
from jax import lax

C = 128
H = 128
N = 256


def place_ends(array, rng, low, largest):
    spot = [jax.random.randint(jax.random.fold_in(rng, axis), (), 0, length) for axis, length in enumerate(array.shape)]
    widest = array.shape.index(max(array.shape))
    neighbour = spot[:widest] + [(spot[widest] + 1) % array.shape[widest]] + spot[widest + 1:]
    return array.at[tuple(spot)].set(low).at[tuple(neighbour)].set(largest)


def levels(own_key, extent, cuts, smallest, top_value):
    factor_of, own = 1.0, jax.random.fold_in(own_key, 6)
    for axis_at, parts in cuts:
        steps = jnp.exp(jax.random.uniform(jax.random.fold_in(own, axis_at), (parts,), jnp.float32, smallest / len(cuts), top_value / len(cuts)))
        factor_of = factor_of * jnp.repeat(steps, extent[axis_at] // parts).reshape([-1 if axis == axis_at else 1 for axis in range(len(extent))])
    return factor_of


def noise(stream_key, dims, scale, most, cuts=(), kind=jnp.bfloat16):
    array = jax.random.normal(stream_key, dims, jnp.float32) * scale
    if len(cuts) > 0:
        array = levels(stream_key, dims, cuts, -0.22, 0.18) * array
    return jnp.clip(array, min=-most, max=most).astype(kind)


def setup_inputs(seed: int = 0) -> dict:
    key_of = jax.random.split(jax.random.key(seed), 13)
    pair_rep = noise(key_of[0], (N, N, C), 1.0, 6.0, ((0, 16), (1, 2)), jnp.float32)
    residue_mask = place_ends((jax.random.randint(key_of[1], (N,), 0, 8) < 7).astype(jnp.int32), jax.random.fold_in(key_of[1], 1), 0, 1)
    pair_gain = jnp.clip(jax.random.uniform(key_of[2], (2, C), jnp.float32, 0.5, 1.5), 0.5, 1.5)
    pair_shift = noise(key_of[3], (2, C), 0.5, 3.0, (), jnp.float32)
    panel_weight = noise(key_of[4], (2, C, 4 * H), C ** -0.5, 0.5)
    panel_bias = noise(key_of[5], (2, 4 * H), 0.5, 3.0, (), jnp.float32)
    gate_weight = noise(key_of[6], (2, C, C), C ** -0.5, 0.5)
    gate_bias = noise(key_of[7], (2, C), 0.5, 3.0, (), jnp.float32)
    hidden_gain = jnp.clip(jax.random.uniform(key_of[8], (2, H), jnp.float32, 0.5, 1.5), 0.5, 1.5)
    hidden_shift = noise(key_of[9], (2, H), 0.5, 3.0, (), jnp.float32)
    output_weight = noise(key_of[10], (2, H, C), H ** -0.5, 0.5)
    output_bias = noise(key_of[11], (2, C), 0.5, 3.0, (), jnp.float32)
    return dict(pair_rep=pair_rep, residue_mask=residue_mask, pair_gain=pair_gain, pair_shift=pair_shift, panel_weight=panel_weight, panel_bias=panel_bias, gate_weight=gate_weight, gate_bias=gate_bias, hidden_gain=hidden_gain, hidden_shift=hidden_shift, output_weight=output_weight, output_bias=output_bias)


PAIR_EPSILON = 1e-05
HIDDEN_EPSILON = 1.0

def layer_norm(values, gain_value, shift_value, along, epsilon):
    center = lax.optimization_barrier(jnp.mean(values, axis=along, keepdims=True))
    offset = values - center
    spread = lax.optimization_barrier(jnp.mean(offset * offset, axis=along, keepdims=True))
    return offset * lax.rsqrt(spread + epsilon) * gain_value + shift_value

def update(current, cell_mask, section_index, pair_gain, pair_shift, panel_weight, panel_bias, gate_weight, gate_bias, hidden_gain, hidden_shift, output_weight, output_bias):
    normed = layer_norm(current, pair_gain[section_index], pair_shift[section_index], -1, PAIR_EPSILON).astype(jnp.bfloat16)
    flattened = normed.reshape(N * N, C)
    weight = panel_weight[section_index]
    biases = panel_bias[section_index]

    def column(which_one):
        result = jnp.dot(flattened, weight[:, which_one * H:(which_one + 1) * H], preferred_element_type=jnp.float32)
        return (result + biases[which_one * H:(which_one + 1) * H]).reshape(N, N, H)
    left_panel = (cell_mask[:, :, None] * jax.nn.sigmoid(column(0)) * column(1)).astype(jnp.bfloat16)
    right_panel = (cell_mask[:, :, None] * jax.nn.sigmoid(column(2)) * column(3)).astype(jnp.bfloat16)
    gate_value = jax.nn.sigmoid(jnp.dot(flattened, gate_weight[section_index], preferred_element_type=jnp.float32) + gate_bias[section_index]).reshape(N, N, C)
    if section_index == 1:
        left_panel = jnp.transpose(left_panel, (1, 0, 2))
        right_panel = jnp.transpose(right_panel, (1, 0, 2))
    left_hidden = jnp.transpose(left_panel, (2, 0, 1)).astype(jnp.float32)
    right_hidden = jnp.transpose(right_panel, (2, 0, 1)).astype(jnp.float32)
    block_rows = math.gcd(N, 128)
    block_count = N // block_rows
    out_weight = output_weight[section_index].astype(jnp.float32)

    def one_block(block_index):
        row_start = block_index * block_rows
        left_rows = lax.dynamic_slice_in_dim(left_hidden, row_start, block_rows, 1)
        products = jnp.einsum('hik,hjk->hij', left_rows, right_hidden, precision=lax.Precision.HIGHEST)
        normed_hidden = layer_norm(products, hidden_gain[section_index][:, None, None], hidden_shift[section_index][:, None, None], 0, HIDDEN_EPSILON).astype(jnp.bfloat16)
        projected = jnp.einsum('hij,hc->ijc', normed_hidden.astype(jnp.float32), out_weight, precision=lax.Precision.HIGHEST)
        gate_rows = lax.dynamic_slice_in_dim(gate_value, row_start, block_rows, 0)
        return gate_rows * (projected + output_bias[section_index])
    updates = lax.map(one_block, jnp.arange(block_count, dtype=jnp.int32))
    return current + updates.reshape(N, N, C)

def reference(pair_rep, residue_mask, pair_gain, pair_shift, panel_weight, panel_bias, gate_weight, gate_bias, hidden_gain, hidden_shift, output_weight, output_bias):
    residue_float = residue_mask.astype(jnp.float32)
    cell_mask = residue_float[:, None] * residue_float[None, :]
    current = pair_rep
    for section_index in range(2):
        current = update(current, cell_mask, section_index, pair_gain, pair_shift, panel_weight, panel_bias, gate_weight, gate_bias, hidden_gain, hidden_shift, output_weight, output_bias)
    return current
```

```python
import functools

import jax
import jax.numpy as jnp
from jax import lax
from jax.experimental import pallas as pl
from jax.experimental.pallas import tpu as pltpu
from jax.sharding import PartitionSpec as P

PAIR_EPSILON = 1e-05
HIDDEN_EPSILON = 1.0
MESH = pl.DeviceIdType.MESH
CHUNKS = 4
LEAD = 3
NAMES = (
    "pair",
    "mask",
    "pair_gain",
    "pair_shift",
    "panel_weight",
    "panel_bias",
    "gate_weight",
    "gate_bias",
    "hidden_gain",
    "hidden_shift",
    "output_weight",
    "output_bias",
)


def normalize(values, axis, epsilon, gain, shift):
    offset = values - jnp.mean(values, axis=axis, keepdims=True)
    spread = jnp.mean(offset * offset, axis=axis, keepdims=True)
    return (offset * lax.rsqrt(spread + epsilon) * gain + shift).astype(jnp.bfloat16)


def kernel(sizes, mask_smem, *refs):
    rows, cols, hidden, row_total, col_total, parts, chunks = sizes
    count = len(NAMES)
    sources = dict(zip(NAMES, refs[:count]))
    out_ref = refs[count]
    held = dict(zip(NAMES, refs[count + 1 : 2 * count + 1]))
    (
        weight_t,
        bias_t,
        affine_t,
        normed_ref,
        stage,
        stage_x,
        gate,
        send_ab,
        recv_a,
        recv_b,
        recv_ab,
        send_x0,
        send_x1,
        recv_x0,
        recv_x1,
        load_sem,
        a_send_sem,
        a_recv_sem,
        b_send_sem,
        b_recv_sem,
        ab_send_sem,
        ab_recv_sem,
        x_send_sem,
        x_recv_sem,
    ) = refs[2 * count + 1 :]
    devices = row_total * col_total
    row_part = row_total // parts
    members = row_part * col_total
    per_slot = hidden // members
    piece = per_slot // chunks
    wide = hidden // chunks
    total = row_total * rows
    part = total // parts
    my_row = lax.axis_index("row")
    my_col = lax.axis_index("ch")
    my_group = my_row // row_part
    my_place = lax.rem(my_row, row_part) * col_total + my_col

    loads = [
        pltpu.make_async_copy(sources[name], held[name], load_sem.at[at])
        for at, name in enumerate(NAMES)
    ]
    for load in loads:
        load.start()

    def partner(distance, step):
        group = lax.rem(my_group + distance, parts)
        place = lax.rem(my_place + step, members)
        return group * row_part + place // col_total, lax.rem(place, col_total), place

    def each(first, body):
        def step_body(step, carry):
            body(step)
            return carry

        steps = members - first
        unroll = max(d for d in (1, 4, 5) if steps % d == 0)
        lax.fori_loop(first, members, step_body, 0, unroll=unroll)

    barrier = pltpu.get_barrier_semaphore()
    for distance in range(parts):

        def greet(step):
            row, col, _ = partner(distance, step)
            pl.semaphore_signal(barrier, inc=1, device_id=(row, col), device_id_type=MESH)

        each(1 if distance == 0 else 0, greet)

    def wait_bytes(ref, sem):
        pltpu.make_async_copy(ref, ref, sem).wait()

    def remote(source, target, send_sem, recv_sem, row, col):
        pltpu.make_async_remote_copy(
            src_ref=source,
            dst_ref=target,
            send_sem=send_sem,
            recv_sem=recv_sem,
            device_id=(row, col),
            device_id_type=MESH,
        ).start()

    row_at = pl.multiple_of(my_row * rows, rows)
    near_at = pl.multiple_of(lax.rem(my_row, row_part) * rows, rows)
    col_at = pl.multiple_of(my_col * cols, cols)

    def panels(chunk, place):
        return pl.ds(chunk * wide + place * piece, piece)

    def send_panels(section, chunk):
        spot = pl.ds(chunk * piece, piece)
        if section == 0:
            a_to = recv_a.at[spot, pl.ds(near_at, rows), pl.ds(col_at, cols)]
            b_to = recv_b.at[spot, pl.ds(row_at, rows), pl.ds(col_at, cols)]

            def far(distance, step):
                row, col, place = partner(distance, step)
                source = send_ab.at[0, 1, panels(chunk, place)]
                remote(
                    source, b_to, b_send_sem.at[distance], b_recv_sem.at[chunk], row, col
                )

            def near(step):
                row, col, place = partner(0, step)
                source = send_ab.at[0, 0, panels(chunk, place)]
                remote(source, a_to, a_send_sem, a_recv_sem.at[chunk], row, col)

            for distance in range(parts - 1, -1, -1):
                each(1 if distance == 0 else 0, functools.partial(far, distance))
            each(1, near)
            own = panels(chunk, my_place)
            pltpu.make_async_copy(send_ab.at[0, 0, own], a_to, a_recv_sem.at[chunk]).start()
            pltpu.make_async_copy(send_ab.at[0, 1, own], b_to, b_recv_sem.at[chunk]).start()
        else:
            to = recv_ab.at[:, spot, pl.ds(near_at, rows), pl.ds(col_at, cols)]

            def both(step):
                row, col, place = partner(0, step)
                source = send_ab.at[1, :, panels(chunk, place)]
                remote(source, to, ab_send_sem, ab_recv_sem.at[chunk], row, col)

            each(1, both)
            own = send_ab.at[1, :, panels(chunk, my_place)]
            pltpu.make_async_copy(own, to, ab_recv_sem.at[chunk]).start()

    def wait_panels(section, chunk):
        spot = pl.ds(chunk * piece, piece)
        if section == 0:
            wait_bytes(recv_a.at[spot], a_recv_sem.at[chunk])
            wait_bytes(recv_b.at[spot], b_recv_sem.at[chunk])
        else:
            wait_bytes(recv_ab.at[:, spot], ab_recv_sem.at[chunk])

    def send_products(section, chunk):
        spot = pl.ds(chunk * piece, piece)
        lands = panels(chunk, my_place)

        def refs_of(row, col):
            to_row = row if section == 1 else lax.rem(row, row_part)
            at = pl.ds(pl.multiple_of(to_row * rows, rows), rows)
            along = pl.ds(pl.multiple_of(col * cols, cols), cols)
            if section == 0:
                return send_x0.at[spot, at, along], recv_x0.at[lands]
            return send_x1.at[spot, at, along], recv_x1.at[my_group, lands]

        def other(distance, step):
            row, col, _ = partner(distance, step)
            source, target = refs_of(row, col)
            remote(
                source,
                target,
                x_send_sem.at[section, distance],
                x_recv_sem.at[section, chunk],
                row,
                col,
            )

        for distance in range(parts - 1 if section == 1 else 0, -1, -1):
            each(1 if distance == 0 else 0, functools.partial(other, distance))
        source, target = refs_of(my_row, my_col)
        pltpu.make_async_copy(source, target, x_recv_sem.at[section, chunk]).start()

    def prepare(section):
        for block in range(4):
            span = slice(block * hidden, (block + 1) * hidden)
            turned = held["panel_weight"][section, :, span].astype(jnp.float32).T
            turned = turned.astype(jnp.bfloat16)
            biases = held["panel_bias"][pl.ds(section, 1), span]
            biases = jnp.broadcast_to(biases, (cols, hidden)).T
            for chunk in range(chunks):
                to = pl.ds((chunk * 4 + block) * wide, wide)
                weight_t[section, to, :] = turned[chunk * wide : (chunk + 1) * wide]
                bias_t[section, to, :] = biases[chunk * wide : (chunk + 1) * wide]

    def prepare_affine(section):
        for at, name in enumerate(("hidden_gain", "hidden_shift")):
            line = held[name][pl.ds(section, 1), :]
            affine_t[section, at] = jnp.broadcast_to(line, (cols, hidden)).T

    def norm_row(section, values):
        return normalize(
            values,
            1,
            PAIR_EPSILON,
            held["pair_gain"][pl.ds(section, 1), :],
            held["pair_shift"][pl.ds(section, 1), :],
        )

    early = [NAMES.index(name) for name in ("pair", "pair_gain", "pair_shift")]
    for at in early:
        loads[at].wait()

    def first_norm(r, carry):
        normed_ref[r] = norm_row(0, held["pair"][r])
        return carry

    lax.fori_loop(0, rows, first_norm, 0, unroll=min(rows, 16))
    for at in range(count):
        if at not in early:
            loads[at].wait()
    prepare(0)
    col_mask = held["mask"][pl.ds(my_col, 1), :].astype(jnp.float32)

    for section in range(2):
        current = held["pair"] if section == 0 else out_ref
        def make(chunk):

            def project(r, carry):
                span = pl.ds(chunk * 4 * wide, 4 * wide)
                features = lax.dot_general(
                    weight_t[section, span, :],
                    normed_ref[r],
                    (((1,), (1,)), ((), ())),
                    preferred_element_type=jnp.float32,
                )
                features = features + bias_t[section, span, :]
                mask = col_mask * mask_smem[my_row * rows + r].astype(jnp.float32)
                for which in range(2):
                    at = 2 * which * wide
                    panel = mask * jax.nn.sigmoid(features[at : at + wide])
                    panel = panel * features[at + wide : at + 2 * wide]
                    stage[which, pl.ds(r, wide, stride=rows), :] = panel
                return carry

            lax.fori_loop(0, rows, project, 0, unroll=min(rows, 16))
            for which in range(2):
                send_ab[section, which, pl.ds(chunk * wide, wide)] = (
                    stage[which].astype(jnp.bfloat16).reshape(wide, rows, cols)
                )
            if section == 0 and chunk == 0:
                pl.semaphore_wait(barrier, devices - 1)
            send_panels(section, chunk)

        def gates(r, carry):
            gate[r] = jax.nn.sigmoid(
                jnp.dot(
                    normed_ref[r],
                    held["gate_weight"][section],
                    preferred_element_type=jnp.float32,
                )
                + held["gate_bias"][pl.ds(section, 1), :]
            )
            return carry

        def multiply(chunk):
            wait_panels(section, chunk)
            for h in range(chunk * piece, (chunk + 1) * piece):
                if section == 0:
                    left, right, along, to = recv_a[h], recv_b[h], 1, send_x0
                else:
                    left, right, along, to = recv_ab[0, h], recv_ab[1, h], 0, send_x1
                to[h] = lax.dot_general(
                    left,
                    right,
                    (((along,), (along,)), ((), ())),
                    preferred_element_type=jnp.float32,
                ).astype(jnp.bfloat16)
            send_products(section, chunk)

        lead = chunks if section == 0 else min(LEAD, chunks)
        for chunk in range(lead):
            make(chunk)
        if section == 0:
            lax.fori_loop(0, rows, gates, 0, unroll=min(rows, 16))
            prepare(1)
            prepare_affine(0)
            prepare_affine(1)
        for chunk in range(chunks):
            multiply(chunk)
            if chunk + lead < chunks:
                make(chunk + lead)
        if section == 1:
            lax.fori_loop(0, rows, gates, 0, unroll=min(rows, 16))
        for chunk in range(chunks):
            spot = pl.ds(chunk * wide, wide)
            if section == 0:
                wait_bytes(recv_x0.at[spot], x_recv_sem.at[0, chunk])
                got = recv_x0[spot].astype(jnp.float32)
            else:
                wait_bytes(recv_x1.at[:, spot], x_recv_sem.at[1, chunk])
                got = recv_x1[0, spot].astype(jnp.float32)
                for other in range(1, parts):
                    got = got + recv_x1[other, spot].astype(jnp.float32)
            stage_x[pl.ds(chunk * wide * rows, wide * rows), :] = got.reshape(wide * rows, cols)

        def finish(r, carry):
            normed = normalize(
                stage_x[pl.ds(r, hidden, stride=rows), :],
                0,
                HIDDEN_EPSILON,
                affine_t[section, 0],
                affine_t[section, 1],
            )
            projected = lax.dot_general(
                normed,
                held["output_weight"][section],
                (((0,), (0,)), ((), ())),
                preferred_element_type=jnp.float32,
            )
            projected = projected + held["output_bias"][pl.ds(section, 1), :]
            updated = current[r] + gate[r] * projected
            out_ref[r] = updated
            if section == 0:
                normed_ref[r] = norm_row(1, updated)
            return carry

        lax.fori_loop(0, rows, finish, 0, unroll=min(rows, 16))

    one = hidden - per_slot
    wait_bytes(send_ab.at[0, 0, pl.ds(0, one)], a_send_sem)
    wait_bytes(send_ab.at[1, :, pl.ds(0, one)], ab_send_sem)
    for distance in range(parts):
        amount = one if distance == 0 else hidden
        wait_bytes(send_ab.at[0, 1, pl.ds(0, amount)], b_send_sem.at[distance])
        wait_bytes(send_ab.at[0, 1, pl.ds(0, amount)], x_send_sem.at[1, distance])
    wait_bytes(recv_x0.at[pl.ds(0, one)], x_send_sem.at[0, 0])


def local(row_total, col_total, pair_rep, residue_mask, *parameters):
    rows, cols, channels = pair_rep.shape
    hidden = parameters[2].shape[2] // 4
    parts = max(2, row_total * col_total // hidden)
    members = row_total * col_total // parts
    per_slot = hidden // members
    chunks = min(CHUNKS, per_slot)
    wide = hidden // chunks
    total = row_total * rows
    part = total // parts
    sizes = (rows, cols, hidden, row_total, col_total, parts, chunks)
    bf16, f32 = jnp.bfloat16, jnp.float32
    dma = pltpu.SemaphoreType.DMA
    arrays = (pair_rep, residue_mask.reshape(col_total, cols), *parameters)
    return pl.pallas_call(
        functools.partial(kernel, sizes),
        out_shape=pltpu.VMEM((rows, cols, channels), f32),
        in_specs=[pl.BlockSpec(memory_space=pltpu.SMEM)]
        + [pl.BlockSpec(memory_space=pltpu.HBM)] * len(arrays),
        out_specs=pl.BlockSpec(memory_space=pltpu.VMEM),
        scratch_shapes=[pltpu.VMEM(array.shape, array.dtype) for array in arrays]
        + [
            pltpu.VMEM((2, 4 * hidden, channels), bf16),
            pltpu.VMEM((2, 4 * hidden, cols), f32),
            pltpu.VMEM((2, 2, hidden, cols), f32),
            pltpu.VMEM((rows, cols, channels), bf16),
            pltpu.VMEM((2, wide * rows, cols), f32),
            pltpu.VMEM((hidden * rows, cols), f32),
            pltpu.VMEM((rows, cols, channels), f32),
            pltpu.VMEM((2, 2, hidden, rows, cols), bf16),
            pltpu.VMEM((per_slot, part, total), bf16),
            pltpu.VMEM((per_slot, total, total), bf16),
            pltpu.VMEM((2, per_slot, part, total), bf16),
            pltpu.VMEM((per_slot, part, total), bf16),
            pltpu.VMEM((per_slot, total, total), bf16),
            pltpu.VMEM((hidden, rows, cols), bf16),
            pltpu.VMEM((parts, hidden, rows, cols), bf16),
            dma((len(arrays),)),
            dma(()),
            dma((chunks,)),
            dma((parts,)),
            dma((chunks,)),
            dma(()),
            dma((chunks,)),
            dma((2, parts)),
            dma((2, chunks)),
        ],
        compiler_params=pltpu.CompilerParams(collective_id=0, has_side_effects=True),
    )(residue_mask, *arrays)


def solution(mesh):
    return jax.shard_map(
        functools.partial(local, mesh.shape["row"], mesh.shape["ch"]),
        mesh=mesh,
        in_specs=(P("row", "ch", None), P(), P(), P(), P(), P(), P(), P(), P(), P(), P(), P()),
        out_specs=P("row", "ch", None),
        check_vma=False,
    )
```

```python
import functools

import jax
import jax.numpy as jnp
from jax import lax
from jax.experimental import pallas as pl
from jax.experimental.pallas import tpu as pltpu
from jax.sharding import PartitionSpec as P

PAIR_EPSILON = 1e-05
HIDDEN_EPSILON = 1.0
MESH = pl.DeviceIdType.MESH
CHUNKS = 4
LEAD = 3
NAMES = (
    "pair",
    "mask",
    "pair_gain",
    "pair_shift",
    "panel_weight",
    "panel_bias",
    "gate_weight",
    "gate_bias",
    "hidden_gain",
    "hidden_shift",
    "output_weight",
    "output_bias",
)


def normalize(values, axis, epsilon, gain, shift):
    offset = values - jnp.mean(values, axis=axis, keepdims=True)
    spread = jnp.mean(offset * offset, axis=axis, keepdims=True)
    return (offset * lax.rsqrt(spread + epsilon) * gain + shift).astype(jnp.bfloat16)


def splat(line, cols):
    return jnp.broadcast_to(line, (cols, line.shape[1])).T


def turn(weight):
    return weight.astype(jnp.float32).T.astype(jnp.bfloat16)


def kernel(sizes, mask_smem, *refs):
    rows, cols, hidden, row_total, col_total, parts, chunks, halves = sizes
    count = len(NAMES)
    sources = dict(zip(NAMES, refs[:count]))
    out_ref = refs[count]
    held = dict(zip(NAMES, refs[count + 1 : 2 * count + 1]))
    (
        weight_t,
        bias_t,
        gate_t,
        output_t,
        lines_t,
        affine_t,
        normed_ref,
        stage,
        stage_x,
        pair_t,
        gate,
        send_ab0,
        send_ab1,
        recv_a,
        recv_b,
        recv_ab,
        send_x0,
        send_x1,
        recv_x0,
        recv_x1,
        load_sem,
        a_send_sem,
        a_recv_sem,
        b_send_sem,
        b_recv_sem,
        ab_send_sem,
        ab_recv_sem,
        x0_send_sem,
        x0_recv_sem,
        x1_send_sem,
        x1_recv_sem,
    ) = refs[2 * count + 1 :]
    devices = row_total * col_total
    row_part = row_total // parts
    members = row_part * col_total
    per_slot = hidden // members
    piece = per_slot // chunks
    wide = hidden // chunks
    sub = rows // halves
    tiles = piece // halves
    my_row = lax.axis_index("row")
    my_col = lax.axis_index("ch")
    my_group = my_row // row_part
    my_near = lax.rem(my_row, row_part)
    my_place = my_near * col_total + my_col

    loads = [
        pltpu.make_async_copy(sources[name], held[name], load_sem.at[at])
        for at, name in enumerate(NAMES)
    ]
    for load in loads:
        load.start()

    def partner(distance, step):
        group = lax.rem(my_group + distance, parts)
        place = lax.rem(my_place + step, members)
        return group * row_part + place // col_total, lax.rem(place, col_total), place

    def each(first, body):
        def step_body(step, carry):
            body(step)
            return carry

        steps = members - first
        unroll = max(d for d in (1, 4, 5) if steps % d == 0)
        lax.fori_loop(first, members, step_body, 0, unroll=unroll)

    barrier = pltpu.get_barrier_semaphore()
    for distance in range(parts):

        def greet(step):
            row, col, _ = partner(distance, step)
            pl.semaphore_signal(barrier, inc=1, device_id=(row, col), device_id_type=MESH)

        each(1 if distance == 0 else 0, greet)

    def wait_bytes(ref, sem):
        pltpu.make_async_copy(ref, ref, sem).wait()

    def remote(source, target, send_sem, recv_sem, row, col):
        pltpu.make_async_remote_copy(
            src_ref=source,
            dst_ref=target,
            send_sem=send_sem,
            recv_sem=recv_sem,
            device_id=(row, col),
            device_id_type=MESH,
        ).start()

    row_at = pl.multiple_of(my_row * rows, rows)
    near_at = pl.multiple_of(my_near * rows, rows)
    col_at = pl.multiple_of(my_col * cols, cols)

    def panels(chunk, place):
        return pl.ds(chunk * wide + place * piece, piece)

    def send_first_panels(chunk):
        spot = pl.ds(chunk * piece, piece)
        a_to = recv_a.at[spot, pl.ds(near_at, rows), pl.ds(col_at, cols)]
        b_to = recv_b.at[spot, pl.ds(row_at, rows), pl.ds(col_at, cols)]

        def far(distance, step):
            row, col, place = partner(distance, step)
            source = send_ab0.at[1, panels(chunk, place)]
            remote(source, b_to, b_send_sem.at[distance], b_recv_sem.at[chunk], row, col)

        def near(step):
            row, col, place = partner(0, step)
            source = send_ab0.at[0, panels(chunk, place)]
            remote(source, a_to, a_send_sem, a_recv_sem.at[chunk], row, col)

        for distance in range(parts - 1, -1, -1):
            each(1 if distance == 0 else 0, functools.partial(far, distance))
        each(1, near)
        own = panels(chunk, my_place)
        pltpu.make_async_copy(send_ab0.at[0, own], a_to, a_recv_sem.at[chunk]).start()
        pltpu.make_async_copy(send_ab0.at[1, own], b_to, b_recv_sem.at[chunk]).start()

    def send_second_panels(half, chunk):
        to = recv_ab.at[
            :, pl.ds(chunk * tiles, tiles), half, my_near, :, pl.ds(col_at, cols)
        ]

        def source_of(place):
            return send_ab1.at[:, half, pl.ds((chunk * members + place) * tiles, tiles)]

        def both(step):
            row, col, place = partner(0, step)
            remote(source_of(place), to, ab_send_sem, ab_recv_sem.at[chunk], row, col)

        each(1, both)
        pltpu.make_async_copy(source_of(my_place), to, ab_recv_sem.at[chunk]).start()

    def send_first_products(half, first, amount):
        lands = recv_x0.at[half, pl.ds(first, amount), pl.ds(my_place * tiles, tiles)]

        def source_of(row, col):
            along = pl.ds(pl.multiple_of(col * cols, cols), cols)
            return send_x0.at[
                half, pl.ds(first, amount), :, lax.rem(row, row_part), :, along
            ]

        def other(step):
            row, col, _ = partner(0, step)
            remote(source_of(row, col), lands, x0_send_sem, x0_recv_sem.at[half], row, col)

        each(1, other)
        own = source_of(my_row, my_col)
        pltpu.make_async_copy(own, lands, x0_recv_sem.at[half]).start()

    def send_second_products(chunk):
        spot = pl.ds(chunk * piece, piece)
        lands = recv_x1.at[my_group, panels(chunk, my_place)]

        def source_of(row, col):
            at = pl.ds(pl.multiple_of(row * rows, rows), rows)
            along = pl.ds(pl.multiple_of(col * cols, cols), cols)
            return send_x1.at[spot, at, along]

        def other(distance, step):
            row, col, _ = partner(distance, step)
            remote(
                source_of(row, col),
                lands,
                x1_send_sem.at[distance],
                x1_recv_sem.at[chunk],
                row,
                col,
            )

        for distance in range(parts - 1, -1, -1):
            each(1 if distance == 0 else 0, functools.partial(other, distance))
        own = source_of(my_row, my_col)
        pltpu.make_async_copy(own, lands, x1_recv_sem.at[chunk]).start()

    def prepare(section):
        for block in range(4):
            span = slice(block * hidden, (block + 1) * hidden)
            turned = turn(held["panel_weight"][section, :, span])
            biases = splat(held["panel_bias"][pl.ds(section, 1), span], cols)
            for chunk in range(chunks):
                to = pl.ds((chunk * 4 + block) * wide, wide)
                weight_t[section, to, :] = turned[chunk * wide : (chunk + 1) * wide]
                bias_t[section, to, :] = biases[chunk * wide : (chunk + 1) * wide]

    def prepare_lines():
        gate_t[...] = turn(held["gate_weight"][0])
        output_t[...] = turn(held["output_weight"][0])
        names = (("gate_bias", 0), ("output_bias", 0), ("pair_gain", 1), ("pair_shift", 1))
        for at, (name, section) in enumerate(names):
            lines_t[at] = splat(held[name][pl.ds(section, 1), :], cols)
        for section in range(2):
            for at, name in enumerate(("hidden_gain", "hidden_shift")):
                line = splat(held[name][pl.ds(section, 1), :], cols)
                affine_t[section, at] = jnp.broadcast_to(line[:, None, :], (hidden, sub, cols))

    def loop(first, steps, body):
        def step_body(r, carry):
            body(r)
            return carry

        lax.fori_loop(first, first + steps, step_body, 0, unroll=min(steps, 16))

    early = [NAMES.index(name) for name in ("pair", "pair_gain", "pair_shift")]
    for at in range(count):
        if at not in early:
            loads[at].wait()
    with jax.named_scope("prep0"):
        prepare(0)
    for at in early:
        loads[at].wait()

    def first_norm(r):
        normed_ref[r] = normalize(
            held["pair"][r],
            1,
            PAIR_EPSILON,
            held["pair_gain"][pl.ds(0, 1), :],
            held["pair_shift"][pl.ds(0, 1), :],
        )

    with jax.named_scope("norm0"):
        loop(0, rows, first_norm)
    col_mask = held["mask"][pl.ds(my_col, 1), :].astype(jnp.float32)

    def project(section, chunk, height, first, r):
        span = pl.ds(chunk * 4 * wide, 4 * wide)
        features = lax.dot_general(
            weight_t[section, span, :],
            normed_ref[r],
            (((1,), (1 - section,)), ((), ())),
            preferred_element_type=jnp.float32,
        )
        features = features + bias_t[section, span, :]
        mask = col_mask * mask_smem[my_row * rows + r].astype(jnp.float32)
        for which in range(2):
            at = 2 * which * wide
            panel = mask * jax.nn.sigmoid(features[at : at + wide])
            panel = panel * features[at + wide : at + 2 * wide]
            stage[which, pl.ds(r - first, wide, stride=height), :] = panel

    def make_first(chunk):
        loop(0, rows, functools.partial(project, 0, chunk, rows, 0))
        for which in range(2):
            send_ab0[which, pl.ds(chunk * wide, wide)] = (
                stage[which].astype(jnp.bfloat16).reshape(wide, rows, cols)
            )
        if chunk == 0:
            with jax.named_scope("barrier"):
                pl.semaphore_wait(barrier, devices - 1)
        send_first_panels(chunk)

    def make_second(half, chunk):
        loop(half * sub, sub, functools.partial(project, 1, chunk, sub, half * sub))
        for which in range(2):
            made = stage[which, pl.ds(0, wide * sub), :].astype(jnp.bfloat16)
            send_ab1[which, half, pl.ds(chunk * members * tiles, members * tiles)] = (
                made.reshape(members * tiles, rows, cols)
            )
        send_second_panels(half, chunk)

    def first_gates(r):
        pair_t[r] = held["pair"][r].T
        features = lax.dot_general(
            gate_t[...],
            normed_ref[r],
            (((1,), (1,)), ((), ())),
            preferred_element_type=jnp.float32,
        )
        gate[r] = jax.nn.sigmoid(features + lines_t[0])

    def second_gates(r):
        held["pair"][r] = pair_t[r].T
        features = lax.dot_general(
            normed_ref[r],
            held["gate_weight"][1],
            (((0,), (0,)), ((), ())),
            preferred_element_type=jnp.float32,
        )
        gate[r] = jax.nn.sigmoid(features + held["gate_bias"][pl.ds(1, 1), :])

    def multiply_first(chunk):
        spot = pl.ds(chunk * piece, piece)
        with jax.named_scope(f"waitab0_{chunk}"):
            wait_bytes(recv_a.at[spot], a_recv_sem.at[chunk])
            wait_bytes(recv_b.at[spot], b_recv_sem.at[chunk])
        for tile in range(tiles):
            products = []
            for h in range(halves):
                at = chunk * piece + tile * halves + h
                product = lax.dot_general(
                    recv_a[at],
                    recv_b[at],
                    (((1,), (1,)), ((), ())),
                    preferred_element_type=jnp.float32,
                )
                products.append(product.reshape(row_part, halves, sub, product.shape[1]))
            for half in range(halves):
                packed = jnp.concatenate([product[:, half] for product in products], axis=1)
                send_x0[half, chunk, tile] = packed.astype(jnp.bfloat16)

    def multiply_second(chunk):
        spot = pl.ds(chunk * tiles, tiles)
        with jax.named_scope(f"waitab1_{chunk}"):
            wait_bytes(recv_ab.at[:, spot], ab_recv_sem.at[chunk])
        for tile in range(tiles):
            sides = []
            for which in range(2):
                got = recv_ab[which, chunk * tiles + tile].astype(jnp.float32)
                got = got.reshape(halves * row_part, halves, sub, got.shape[-1])
                sides.append(got)
            for h in range(halves):
                left, right = (
                    side[:, h]
                    .reshape(row_part * rows, side.shape[-1])
                    .astype(jnp.bfloat16)
                    for side in sides
                )
                send_x1[chunk * piece + tile * halves + h] = lax.dot_general(
                    left,
                    right,
                    (((0,), (0,)), ((), ())),
                    preferred_element_type=jnp.float32,
                ).astype(jnp.bfloat16)
        send_second_products(chunk)

    def normalize_hidden(section, half):
        values = stage_x[half].reshape(hidden, sub, cols)
        center = jnp.sum(values, axis=0, keepdims=True) * (1.0 / hidden)
        offset = values - center
        spread = jnp.sum(offset * offset, axis=0, keepdims=True) * (1.0 / hidden)
        scale = lax.rsqrt(spread + HIDDEN_EPSILON)
        normed = offset * scale * affine_t[section, 0] + affine_t[section, 1]
        stage_x[half] = normed.reshape(hidden * sub, cols)

    def finish_first(half):
        with jax.named_scope(f"waitx0_{half}"):
            wait_bytes(recv_x0.at[half], x0_recv_sem.at[half])
        with jax.named_scope(f"finish0_{half}"):
            got = recv_x0[half].astype(jnp.float32)
            stage_x[half] = got.reshape(hidden * sub, cols)
            normalize_hidden(0, half)

            def finish(r):
                normed = stage_x[half, pl.ds(r - half * sub, hidden, stride=sub), :]
                projected = jnp.dot(
                    output_t[...],
                    normed.astype(jnp.bfloat16),
                    preferred_element_type=jnp.float32,
                )
                updated = pair_t[r] + gate[r] * (projected + lines_t[1])
                pair_t[r] = updated
                normed_ref[r] = normalize(updated, 0, PAIR_EPSILON, lines_t[2], lines_t[3])

            loop(half * sub, sub, finish)

    for chunk in range(chunks):
        with jax.named_scope(f"make0_{chunk}"):
            make_first(chunk)
    with jax.named_scope("gates0"):
        prepare_lines()
        loop(0, rows, first_gates)
        prepare(1)
    for chunk in range(chunks):
        with jax.named_scope(f"mult0_{chunk}"):
            multiply_first(chunk)
            if chunk == chunks - 2:
                send_first_products(0, 0, chunks - 1)
            if chunk == chunks - 1:
                send_first_products(0, max(chunks - 1, 0), 1)
                for half in range(1, halves):
                    send_first_products(half, 0, chunks)

    lead = min(LEAD, chunks)

    def produce(half, chunk):
        with jax.named_scope(f"make1_{half}_{chunk}"):
            make_second(half, chunk)

    early_chunks = min(2, chunks) if halves > 1 else 0
    for half in range(halves):
        finish_first(half)
        if half < halves - 1:
            for chunk in range(early_chunks):
                produce(half, chunk)
    for chunk in range(lead):
        for half in range(halves):
            if not (half < halves - 1 and chunk < early_chunks):
                produce(half, chunk)
    for chunk in range(chunks):
        with jax.named_scope(f"mult1_{chunk}"):
            multiply_second(chunk)
        if chunk + lead < chunks:
            for half in range(halves):
                produce(half, chunk + lead)
    with jax.named_scope("gates1"):
        loop(0, rows, second_gates)
    for chunk in range(chunks):
        spot = pl.ds(chunk * wide, wide)
        with jax.named_scope(f"waitx1_{chunk}"):
            wait_bytes(recv_x1.at[:, spot], x1_recv_sem.at[chunk])
        got = recv_x1[0, spot].astype(jnp.float32)
        for other in range(1, parts):
            got = got + recv_x1[other, spot].astype(jnp.float32)
        got = got.reshape(wide, halves, sub, cols)
        for half in range(halves):
            stage_x[half, pl.ds(chunk * wide * sub, wide * sub), :] = got[:, half].reshape(
                wide * sub, cols
            )

    with jax.named_scope("finish1"):
        for half in range(halves):
            normalize_hidden(1, half)

            def finish(r):
                normed = stage_x[half, pl.ds(r - half * sub, hidden, stride=sub), :]
                projected = lax.dot_general(
                    normed.astype(jnp.bfloat16),
                    held["output_weight"][1],
                    (((0,), (0,)), ((), ())),
                    preferred_element_type=jnp.float32,
                )
                projected = projected + held["output_bias"][pl.ds(1, 1), :]
                out_ref[r] = held["pair"][r] + gate[r] * projected

            loop(half * sub, sub, finish)

    one = hidden - per_slot
    wait_bytes(send_ab0.at[0, pl.ds(0, one)], a_send_sem)
    wait_bytes(send_ab1.at[:, :, pl.ds(0, one // halves)], ab_send_sem)
    for distance in range(parts):
        amount = one if distance == 0 else hidden
        wait_bytes(send_ab0.at[1, pl.ds(0, amount)], b_send_sem.at[distance])
        wait_bytes(send_ab0.at[1, pl.ds(0, amount)], x1_send_sem.at[distance])
    wait_bytes(send_ab0.at[0, pl.ds(0, one)], x0_send_sem)


def local(row_total, col_total, pair_rep, residue_mask, *parameters):
    rows, cols, channels = pair_rep.shape
    hidden = parameters[2].shape[2] // 4
    parts = max(2, row_total * col_total // hidden)
    members = row_total * col_total // parts
    row_part = row_total // parts
    per_slot = hidden // members
    chunks = min(CHUNKS, per_slot)
    piece = per_slot // chunks
    halves = 2 if piece % 2 == 0 and rows % 16 == 0 else 1
    tiles = piece // halves
    sub = rows // halves
    wide = hidden // chunks
    total = row_total * rows
    part = total // parts
    sizes = (rows, cols, hidden, row_total, col_total, parts, chunks, halves)
    bf16, f32 = jnp.bfloat16, jnp.float32
    dma = pltpu.SemaphoreType.DMA
    arrays = (pair_rep, residue_mask.reshape(col_total, cols), *parameters)
    return pl.pallas_call(
        functools.partial(kernel, sizes),
        out_shape=pltpu.VMEM((rows, cols, channels), f32),
        in_specs=[pl.BlockSpec(memory_space=pltpu.SMEM)]
        + [pl.BlockSpec(memory_space=pltpu.HBM)] * len(arrays),
        out_specs=pl.BlockSpec(memory_space=pltpu.VMEM),
        scratch_shapes=[pltpu.VMEM(array.shape, array.dtype) for array in arrays]
        + [
            pltpu.VMEM((2, 4 * hidden, channels), bf16),
            pltpu.VMEM((2, 4 * hidden, cols), f32),
            pltpu.VMEM((channels, channels), bf16),
            pltpu.VMEM((channels, hidden), bf16),
            pltpu.VMEM((4, channels, cols), f32),
            pltpu.VMEM((2, 2, hidden, sub, cols), f32),
            pltpu.VMEM((rows, cols, channels), bf16),
            pltpu.VMEM((2, wide * rows, cols), f32),
            pltpu.VMEM((halves, hidden * sub, cols), f32),
            pltpu.VMEM((rows, channels, cols), f32),
            pltpu.VMEM((rows, cols, channels), f32),
            pltpu.VMEM((2, hidden, rows, cols), bf16),
            pltpu.VMEM((2, halves, hidden // halves, rows, cols), bf16),
            pltpu.VMEM((per_slot, part, total), bf16),
            pltpu.VMEM((per_slot, total, total), bf16),
            pltpu.VMEM((2, per_slot // halves, halves, row_part, rows, total), bf16),
            pltpu.VMEM((halves, chunks, tiles, row_part, rows, total), bf16),
            pltpu.VMEM((per_slot, total, total), bf16),
            pltpu.VMEM((halves, chunks, members * tiles, rows, cols), bf16),
            pltpu.VMEM((parts, hidden, rows, cols), bf16),
            dma((len(arrays),)),
            dma(()),
            dma((chunks,)),
            dma((parts,)),
            dma((chunks,)),
            dma(()),
            dma((chunks,)),
            dma(()),
            dma((halves,)),
            dma((parts,)),
            dma((chunks,)),
        ],
        compiler_params=pltpu.CompilerParams(collective_id=0, has_side_effects=True),
    )(residue_mask, *arrays)


def solution(mesh):
    return jax.shard_map(
        functools.partial(local, mesh.shape["row"], mesh.shape["ch"]),
        mesh=mesh,
        in_specs=(P("row", "ch", None), P(), P(), P(), P(), P(), P(), P(), P(), P(), P(), P()),
        out_specs=P("row", "ch", None),
        check_vma=False,
    )
```

```python
import functools

import jax
import jax.numpy as jnp
from jax import lax
from jax.experimental import pallas as pl
from jax.experimental.pallas import tpu as pltpu
from jax.sharding import PartitionSpec as P

PAIR_EPSILON = 1e-05
HIDDEN_EPSILON = 1.0
MESH = pl.DeviceIdType.MESH
CHUNKS = 4
LEAD = 3
NAMES = (
    "pair",
    "mask",
    "pair_gain",
    "pair_shift",
    "panel_weight",
    "panel_bias",
    "gate_weight",
    "gate_bias",
    "hidden_gain",
    "hidden_shift",
    "output_weight",
    "output_bias",
)


def normalize(values, axis, epsilon, gain, shift):
    offset = values - jnp.mean(values, axis=axis, keepdims=True)
    spread = jnp.mean(offset * offset, axis=axis, keepdims=True)
    return (offset * lax.rsqrt(spread + epsilon) * gain + shift).astype(jnp.bfloat16)


def splat(line, cols):
    return jnp.broadcast_to(line, (cols, line.shape[1])).T


def turn(weight):
    return weight.astype(jnp.float32).T.astype(jnp.bfloat16)


def kernel(sizes, mask_hbm, *refs):
    rows, cols, hidden, row_total, col_total, parts, chunks, halves = sizes
    count = len(NAMES)
    sources = dict(zip(NAMES, refs[:count]))
    out_ref = refs[count]
    held = dict(zip(NAMES, refs[count + 1 : 2 * count + 1]))
    (
        weight_t,
        bias_t,
        gate_t,
        output_t,
        lines_t,
        affine_t,
        normed_ref,
        stage,
        stage_x,
        pair_t,
        gate,
        send_ab0,
        send_ab1,
        recv_a,
        recv_b,
        recv_ab,
        send_x0,
        send_x1,
        recv_x0,
        recv_x1,
        load_sem,
        a_send_sem,
        a_recv_sem,
        b_send_sem,
        b_recv_sem,
        ab_send_sem,
        ab_recv_sem,
        x0_send_sem,
        x0_recv_sem,
        x1_send_sem,
        x1_recv_sem,
        mask_smem,
        mask_sem,
    ) = refs[2 * count + 1 :]
    devices = row_total * col_total
    row_part = row_total // parts
    members = row_part * col_total
    per_slot = hidden // members
    piece = per_slot // chunks
    wide = hidden // chunks
    sub = rows // halves
    tiles = piece // halves
    my_row = lax.axis_index("row")
    my_col = lax.axis_index("ch")
    my_group = my_row // row_part
    my_near = lax.rem(my_row, row_part)
    my_place = my_near * col_total + my_col

    loads = [
        pltpu.make_async_copy(sources[name], held[name], load_sem.at[at])
        for at, name in enumerate(NAMES)
    ]
    order = ("panel_weight", "pair_gain", "pair_shift", "panel_bias", "mask", "pair")
    urgent = [NAMES.index(name) for name in order]
    later = [at for at in range(count) if at not in urgent]
    mask_load = pltpu.make_async_copy(mask_hbm, mask_smem, mask_sem)
    for at in urgent:
        loads[at].start()
    mask_load.start()
    for at in later:
        loads[at].start()

    def partner(distance, step):
        group = lax.rem(my_group + distance, parts)
        place = lax.rem(my_place + step, members)
        return group * row_part + place // col_total, lax.rem(place, col_total), place

    def each(first, body):
        def step_body(step, carry):
            body(step)
            return carry

        steps = members - first
        unroll = max(d for d in (1, 4, 5) if steps % d == 0)
        lax.fori_loop(first, members, step_body, 0, unroll=unroll)

    barrier = pltpu.get_barrier_semaphore()
    for distance in range(parts):

        def greet(step):
            row, col, _ = partner(distance, step)
            pl.semaphore_signal(barrier, inc=1, device_id=(row, col), device_id_type=MESH)

        each(1 if distance == 0 else 0, greet)

    def wait_bytes(ref, sem):
        pltpu.make_async_copy(ref, ref, sem).wait()

    def remote(source, target, send_sem, recv_sem, row, col):
        pltpu.make_async_remote_copy(
            src_ref=source,
            dst_ref=target,
            send_sem=send_sem,
            recv_sem=recv_sem,
            device_id=(row, col),
            device_id_type=MESH,
        ).start()

    row_at = pl.multiple_of(my_row * rows, rows)
    near_at = pl.multiple_of(my_near * rows, rows)
    col_at = pl.multiple_of(my_col * cols, cols)

    def panels(chunk, place):
        return pl.ds(chunk * wide + place * piece, piece)

    def first_targets(chunk):
        spot = pl.ds(chunk * piece, piece)
        a_to = recv_a.at[spot, pl.ds(near_at, rows), pl.ds(col_at, cols)]
        b_to = recv_b.at[spot, pl.ds(row_at, rows), pl.ds(col_at, cols)]
        return a_to, b_to

    def send_right(distance, chunk):
        _, b_to = first_targets(chunk)

        def right(step):
            row, col, place = partner(distance, step)
            source = send_ab0.at[1, panels(chunk, place)]
            remote(source, b_to, b_send_sem.at[distance], b_recv_sem.at[chunk], row, col)

        each(1 if distance == 0 else 0, right)

    def send_near_panels(chunk):
        a_to, b_to = first_targets(chunk)

        def left(step):
            row, col, place = partner(0, step)
            source = send_ab0.at[0, panels(chunk, place)]
            remote(source, a_to, a_send_sem, a_recv_sem.at[chunk], row, col)

        send_right(0, chunk)
        each(1, left)
        own = panels(chunk, my_place)
        pltpu.make_async_copy(send_ab0.at[0, own], a_to, a_recv_sem.at[chunk]).start()
        pltpu.make_async_copy(send_ab0.at[1, own], b_to, b_recv_sem.at[chunk]).start()

    def send_far_panels(chunk):
        for distance in range(parts - 1, 0, -1):
            send_right(distance, chunk)

    def send_second_panels(half, chunk):
        to = recv_ab.at[
            :, pl.ds(chunk * tiles, tiles), half, my_near, :, pl.ds(col_at, cols)
        ]

        def source_of(place):
            return send_ab1.at[:, half, pl.ds((chunk * members + place) * tiles, tiles)]

        def both(step):
            row, col, place = partner(0, step)
            remote(source_of(place), to, ab_send_sem, ab_recv_sem.at[chunk], row, col)

        each(1, both)
        pltpu.make_async_copy(source_of(my_place), to, ab_recv_sem.at[chunk]).start()

    def send_first_products(half, first, amount):
        lands = recv_x0.at[half, pl.ds(first, amount), pl.ds(my_place * tiles, tiles)]

        def source_of(row, col):
            along = pl.ds(pl.multiple_of(col * cols, cols), cols)
            return send_x0.at[
                half, pl.ds(first, amount), :, lax.rem(row, row_part), :, along
            ]

        def other(step):
            row, col, _ = partner(0, step)
            remote(source_of(row, col), lands, x0_send_sem, x0_recv_sem.at[half], row, col)

        each(1, other)
        own = source_of(my_row, my_col)
        pltpu.make_async_copy(own, lands, x0_recv_sem.at[half]).start()

    def send_second_products(chunk):
        spot = pl.ds(chunk * piece, piece)
        lands = recv_x1.at[my_group, panels(chunk, my_place)]

        def source_of(row, col):
            at = pl.ds(pl.multiple_of(row * rows, rows), rows)
            along = pl.ds(pl.multiple_of(col * cols, cols), cols)
            return send_x1.at[spot, at, along]

        def other(distance, step):
            row, col, _ = partner(distance, step)
            remote(
                source_of(row, col),
                lands,
                x1_send_sem.at[distance],
                x1_recv_sem.at[chunk],
                row,
                col,
            )

        for distance in range(parts - 1, -1, -1):
            each(1 if distance == 0 else 0, functools.partial(other, distance))
        own = source_of(my_row, my_col)
        pltpu.make_async_copy(own, lands, x1_recv_sem.at[chunk]).start()

    def prepare(section):
        for block in range(4):
            span = slice(block * hidden, (block + 1) * hidden)
            turned = turn(held["panel_weight"][section, :, span])
            biases = splat(held["panel_bias"][pl.ds(section, 1), span], cols)
            for chunk in range(chunks):
                to = pl.ds((chunk * 4 + block) * wide, wide)
                weight_t[section, to, :] = turned[chunk * wide : (chunk + 1) * wide]
                bias_t[section, to, :] = biases[chunk * wide : (chunk + 1) * wide]

    def prepare_lines():
        gate_t[...] = turn(held["gate_weight"][0])
        output_t[...] = turn(held["output_weight"][0])
        names = (("gate_bias", 0), ("output_bias", 0), ("pair_gain", 1), ("pair_shift", 1))
        for at, (name, section) in enumerate(names):
            lines_t[2 + at] = splat(held[name][pl.ds(section, 1), :], cols)
        for section in range(2):
            for at, name in enumerate(("hidden_gain", "hidden_shift")):
                line = splat(held[name][pl.ds(section, 1), :], cols)
                affine_t[section, at] = jnp.broadcast_to(line[:, None, :], (hidden, sub, cols))

    def loop(first, steps, body):
        def step_body(r, carry):
            body(r)
            return carry

        lax.fori_loop(first, first + steps, step_body, 0, unroll=min(steps, 16))

    for at in urgent[:-1]:
        loads[at].wait()
    with jax.named_scope("prep0"):
        for at, name in enumerate(("pair_gain", "pair_shift")):
            lines_t[at] = splat(held[name][pl.ds(0, 1), :], cols)
        prepare(0)
    mask_load.wait()
    loads[urgent[-1]].wait()

    def first_norm(r):
        values = held["pair"][r].T
        pair_t[r] = values
        normed_ref[r] = normalize(values, 0, PAIR_EPSILON, lines_t[0], lines_t[1])

    with jax.named_scope("norm0"):
        loop(0, rows, first_norm)
    col_mask = held["mask"][pl.ds(my_col, 1), :].astype(jnp.float32)

    def project(section, chunk, height, first, r):
        span = pl.ds(chunk * 4 * wide, 4 * wide)
        features = lax.dot_general(
            weight_t[section, span, :],
            normed_ref[r],
            (((1,), (0,)), ((), ())),
            preferred_element_type=jnp.float32,
        )
        features = features + bias_t[section, span, :]
        mask = col_mask * mask_smem[my_row * rows + r].astype(jnp.float32)
        for which in range(2):
            at = 2 * which * wide
            panel = mask * jax.nn.sigmoid(features[at : at + wide])
            panel = panel * features[at + wide : at + 2 * wide]
            stage[which, pl.ds(r - first, wide, stride=height), :] = panel

    def make_first(chunk):
        loop(0, rows, functools.partial(project, 0, chunk, rows, 0))
        for which in range(2):
            send_ab0[which, pl.ds(chunk * wide, wide)] = (
                stage[which].astype(jnp.bfloat16).reshape(wide, rows, cols)
            )
        if chunk == 0:
            with jax.named_scope("barrier"):
                pl.semaphore_wait(barrier, devices - 1)
        send_far_panels(chunk)
        send_near_panels(chunk)

    def make_second(half, chunk):
        loop(half * sub, sub, functools.partial(project, 1, chunk, sub, half * sub))
        for which in range(2):
            made = stage[which, pl.ds(0, wide * sub), :].astype(jnp.bfloat16)
            send_ab1[which, half, pl.ds(chunk * members * tiles, members * tiles)] = (
                made.reshape(members * tiles, rows, cols)
            )
        send_second_panels(half, chunk)

    def first_gates(r):
        features = jnp.dot(gate_t[...], normed_ref[r], preferred_element_type=jnp.float32)
        gate[r] = jax.nn.sigmoid(features + lines_t[2])

    def second_gates(r):
        held["pair"][r] = pair_t[r].T
        features = lax.dot_general(
            normed_ref[r],
            held["gate_weight"][1],
            (((0,), (0,)), ((), ())),
            preferred_element_type=jnp.float32,
        )
        gate[r] = jax.nn.sigmoid(features + held["gate_bias"][pl.ds(1, 1), :])

    def multiply_first(chunk):
        spot = pl.ds(chunk * piece, piece)
        with jax.named_scope(f"waitab0_{chunk}"):
            wait_bytes(recv_a.at[spot], a_recv_sem.at[chunk])
            wait_bytes(recv_b.at[spot], b_recv_sem.at[chunk])
        for tile in range(tiles):
            products = []
            for h in range(halves):
                at = chunk * piece + tile * halves + h
                product = lax.dot_general(
                    recv_a[at],
                    recv_b[at],
                    (((1,), (1,)), ((), ())),
                    preferred_element_type=jnp.float32,
                )
                products.append(product.reshape(row_part, halves, sub, product.shape[1]))
            for half in range(halves):
                packed = jnp.concatenate([product[:, half] for product in products], axis=1)
                send_x0[half, chunk, tile] = packed.astype(jnp.bfloat16)

    def multiply_second(chunk):
        spot = pl.ds(chunk * tiles, tiles)
        with jax.named_scope(f"waitab1_{chunk}"):
            wait_bytes(recv_ab.at[:, spot], ab_recv_sem.at[chunk])
        for tile in range(tiles):
            sides = []
            for which in range(2):
                got = recv_ab[which, chunk * tiles + tile].astype(jnp.float32)
                got = got.reshape(halves * row_part, halves, sub, got.shape[-1])
                sides.append(got)
            for h in range(halves):
                left, right = (
                    side[:, h]
                    .reshape(row_part * rows, side.shape[-1])
                    .astype(jnp.bfloat16)
                    for side in sides
                )
                send_x1[chunk * piece + tile * halves + h] = lax.dot_general(
                    left,
                    right,
                    (((0,), (0,)), ((), ())),
                    preferred_element_type=jnp.float32,
                ).astype(jnp.bfloat16)
        send_second_products(chunk)

    def normalize_hidden(section, half):
        values = stage_x[half].reshape(hidden, sub, cols)
        center = jnp.sum(values, axis=0, keepdims=True) * (1.0 / hidden)
        offset = values - center
        spread = jnp.sum(offset * offset, axis=0, keepdims=True) * (1.0 / hidden)
        scale = lax.rsqrt(spread + HIDDEN_EPSILON)
        normed = offset * scale * affine_t[section, 0] + affine_t[section, 1]
        stage_x[half] = normed.reshape(hidden * sub, cols)

    def finish_first(half):
        with jax.named_scope(f"waitx0_{half}"):
            wait_bytes(recv_x0.at[half], x0_recv_sem.at[half])
        with jax.named_scope(f"finish0_{half}"):
            got = recv_x0[half].astype(jnp.float32)
            stage_x[half] = got.reshape(hidden * sub, cols)
            normalize_hidden(0, half)

            def finish(r):
                normed = stage_x[half, pl.ds(r - half * sub, hidden, stride=sub), :]
                projected = jnp.dot(
                    output_t[...],
                    normed.astype(jnp.bfloat16),
                    preferred_element_type=jnp.float32,
                )
                updated = pair_t[r] + gate[r] * (projected + lines_t[3])
                pair_t[r] = updated
                normed_ref[r] = normalize(updated, 0, PAIR_EPSILON, lines_t[4], lines_t[5])

            loop(half * sub, sub, finish)

    for chunk in range(chunks):
        with jax.named_scope(f"make0_{chunk}"):
            make_first(chunk)
    for at in later:
        loads[at].wait()
    with jax.named_scope("gates0"):
        prepare_lines()
        loop(0, rows, first_gates)
        prepare(1)
    for chunk in range(chunks):
        with jax.named_scope(f"mult0_{chunk}"):
            multiply_first(chunk)
            if chunk == chunks - 2:
                send_first_products(0, 0, chunks - 1)
                for half in range(1, halves):
                    send_first_products(half, 0, chunks - 1)
            if chunk == chunks - 1:
                for half in range(halves):
                    send_first_products(half, chunk, 1)

    lead = min(LEAD, chunks)

    def produce(half, chunk):
        with jax.named_scope(f"make1_{half}_{chunk}"):
            make_second(half, chunk)

    early_chunks = min(1, chunks) if halves > 1 else 0
    for half in range(halves):
        finish_first(half)
        if half < halves - 1:
            for chunk in range(early_chunks):
                produce(half, chunk)
    for chunk in range(lead):
        for half in range(halves):
            if not (half < halves - 1 and chunk < early_chunks):
                produce(half, chunk)
    for chunk in range(chunks):
        with jax.named_scope(f"mult1_{chunk}"):
            multiply_second(chunk)
        if chunk + lead < chunks:
            for half in range(halves):
                produce(half, chunk + lead)
    with jax.named_scope("gates1"):
        loop(0, rows, second_gates)
    for chunk in range(chunks):
        spot = pl.ds(chunk * wide, wide)
        with jax.named_scope(f"waitx1_{chunk}"):
            wait_bytes(recv_x1.at[:, spot], x1_recv_sem.at[chunk])
        got = recv_x1[0, spot].astype(jnp.float32)
        for other in range(1, parts):
            got = got + recv_x1[other, spot].astype(jnp.float32)
        got = got.reshape(wide, halves, sub, cols)
        for half in range(halves):
            stage_x[half, pl.ds(chunk * wide * sub, wide * sub), :] = got[:, half].reshape(
                wide * sub, cols
            )

    with jax.named_scope("finish1"):
        for half in range(halves):
            normalize_hidden(1, half)

            def finish(r):
                normed = stage_x[half, pl.ds(r - half * sub, hidden, stride=sub), :]
                projected = lax.dot_general(
                    normed.astype(jnp.bfloat16),
                    held["output_weight"][1],
                    (((0,), (0,)), ((), ())),
                    preferred_element_type=jnp.float32,
                )
                projected = projected + held["output_bias"][pl.ds(1, 1), :]
                out_ref[r] = held["pair"][r] + gate[r] * projected

            loop(half * sub, sub, finish)

    one = hidden - per_slot
    wait_bytes(send_ab0.at[0, pl.ds(0, one)], a_send_sem)
    wait_bytes(send_ab1.at[:, :, pl.ds(0, one // halves)], ab_send_sem)
    for distance in range(parts):
        amount = one if distance == 0 else hidden
        wait_bytes(send_ab0.at[1, pl.ds(0, amount)], b_send_sem.at[distance])
        wait_bytes(send_ab0.at[1, pl.ds(0, amount)], x1_send_sem.at[distance])
    wait_bytes(send_ab0.at[0, pl.ds(0, one)], x0_send_sem)


def local(row_total, col_total, pair_rep, residue_mask, *parameters):
    rows, cols, channels = pair_rep.shape
    hidden = parameters[2].shape[2] // 4
    parts = max(2, row_total * col_total // hidden)
    members = row_total * col_total // parts
    row_part = row_total // parts
    per_slot = hidden // members
    chunks = min(CHUNKS, per_slot)
    piece = per_slot // chunks
    halves = 2 if piece % 2 == 0 and rows % 16 == 0 else 1
    tiles = piece // halves
    sub = rows // halves
    wide = hidden // chunks
    total = row_total * rows
    part = total // parts
    sizes = (rows, cols, hidden, row_total, col_total, parts, chunks, halves)
    bf16, f32 = jnp.bfloat16, jnp.float32
    dma = pltpu.SemaphoreType.DMA
    arrays = (pair_rep, residue_mask.reshape(col_total, cols), *parameters)
    return pl.pallas_call(
        functools.partial(kernel, sizes),
        out_shape=pltpu.VMEM((rows, cols, channels), f32),
        in_specs=[pl.BlockSpec(memory_space=pltpu.HBM)] * (1 + len(arrays)),
        out_specs=pl.BlockSpec(memory_space=pltpu.VMEM),
        scratch_shapes=[pltpu.VMEM(array.shape, array.dtype) for array in arrays]
        + [
            pltpu.VMEM((2, 4 * hidden, channels), bf16),
            pltpu.VMEM((2, 4 * hidden, cols), f32),
            pltpu.VMEM((channels, channels), bf16),
            pltpu.VMEM((channels, hidden), bf16),
            pltpu.VMEM((6, channels, cols), f32),
            pltpu.VMEM((2, 2, hidden, sub, cols), f32),
            pltpu.VMEM((rows, channels, cols), bf16),
            pltpu.VMEM((2, wide * rows, cols), f32),
            pltpu.VMEM((halves, hidden * sub, cols), f32),
            pltpu.VMEM((rows, channels, cols), f32),
            pltpu.VMEM((rows, cols, channels), f32),
            pltpu.VMEM((2, hidden, rows, cols), bf16),
            pltpu.VMEM((2, halves, hidden // halves, rows, cols), bf16),
            pltpu.VMEM((per_slot, part, total), bf16),
            pltpu.VMEM((per_slot, total, total), bf16),
            pltpu.VMEM((2, per_slot // halves, halves, row_part, rows, total), bf16),
            pltpu.VMEM((halves, chunks, tiles, row_part, rows, total), bf16),
            pltpu.VMEM((per_slot, total, total), bf16),
            pltpu.VMEM((halves, chunks, members * tiles, rows, cols), bf16),
            pltpu.VMEM((parts, hidden, rows, cols), bf16),
            dma((len(arrays),)),
            dma(()),
            dma((chunks,)),
            dma((parts,)),
            dma((chunks,)),
            dma(()),
            dma((chunks,)),
            dma(()),
            dma((halves,)),
            dma((parts,)),
            dma((chunks,)),
            pltpu.SMEM(residue_mask.shape, residue_mask.dtype),
            dma(()),
        ],
        compiler_params=pltpu.CompilerParams(collective_id=0, has_side_effects=True),
    )(residue_mask, *arrays)


def solution(mesh):
    return jax.shard_map(
        functools.partial(local, mesh.shape["row"], mesh.shape["ch"]),
        mesh=mesh,
        in_specs=(P("row", "ch", None), P(), P(), P(), P(), P(), P(), P(), P(), P(), P(), P()),
        out_specs=P("row", "ch", None),
        check_vma=False,
    )
```

```python
import functools

import jax
import jax.numpy as jnp
from jax import lax
from jax.experimental import pallas as pl
from jax.experimental.pallas import tpu as pltpu
from jax.sharding import PartitionSpec as P

PAIR_EPSILON = 1e-05
HIDDEN_EPSILON = 1.0
MESH = pl.DeviceIdType.MESH
CHUNKS = 4
LEAD = 4
NAMES = (
    "pair",
    "mask",
    "pair_gain",
    "pair_shift",
    "panel_weight",
    "panel_bias",
    "gate_weight",
    "gate_bias",
    "hidden_gain",
    "hidden_shift",
    "output_weight",
    "output_bias",
)


def normalize(values, axis, epsilon, gain, shift):
    offset = values - jnp.mean(values, axis=axis, keepdims=True)
    spread = jnp.mean(offset * offset, axis=axis, keepdims=True)
    return (offset * lax.rsqrt(spread + epsilon) * gain + shift).astype(jnp.bfloat16)


def splat(line, cols):
    return jnp.broadcast_to(line, (cols, line.shape[1])).T


def turn(weight):
    return weight.astype(jnp.float32).T.astype(jnp.bfloat16)


def kernel(sizes, mask_hbm, *refs):
    rows, cols, hidden, row_total, col_total, parts, chunks, halves = sizes
    count = len(NAMES)
    sources = dict(zip(NAMES, refs[:count]))
    out_ref = refs[count]
    held = dict(zip(NAMES, refs[count + 1 : 2 * count + 1]))
    (
        weight_t,
        bias_t,
        gate_t,
        output_t,
        lines_t,
        affine_t,
        normed_ref,
        stage,
        stage_x,
        pair_t,
        gate,
        send_ab0,
        send_ab1,
        recv_a,
        recv_b,
        recv_ab,
        send_x0,
        send_x1,
        recv_x0,
        recv_x1,
        load_sem,
        a_send_sem,
        a_recv_sem,
        b_send_sem,
        b_recv_sem,
        ab_send_sem,
        ab_recv_sem,
        x0_send_sem,
        x0_recv_sem,
        x1_send_sem,
        x1_recv_sem,
        mask_smem,
        mask_sem,
    ) = refs[2 * count + 1 :]
    devices = row_total * col_total
    row_part = row_total // parts
    members = row_part * col_total
    per_slot = hidden // members
    piece = per_slot // chunks
    wide = hidden // chunks
    sub = rows // halves
    tiles = piece // halves
    my_row = lax.axis_index("row")
    my_col = lax.axis_index("ch")
    my_group = my_row // row_part
    my_near = lax.rem(my_row, row_part)
    my_place = my_near * col_total + my_col

    loads = [
        pltpu.make_async_copy(sources[name], held[name], load_sem.at[at])
        for at, name in enumerate(NAMES)
    ]
    order = ("panel_weight", "pair_gain", "pair_shift", "panel_bias", "mask", "pair")
    urgent = [NAMES.index(name) for name in order]
    later = [at for at in range(count) if at not in urgent]
    mask_load = pltpu.make_async_copy(mask_hbm, mask_smem, mask_sem)
    for at in urgent:
        loads[at].start()
    mask_load.start()
    for at in later:
        loads[at].start()

    def partner(distance, step):
        group = lax.rem(my_group + distance, parts)
        place = lax.rem(my_place + step, members)
        return group * row_part + place // col_total, lax.rem(place, col_total), place

    def each(first, body):
        def step_body(step, carry):
            body(step)
            return carry

        steps = members - first
        unroll = max(d for d in (1, 4, 5) if steps % d == 0)
        lax.fori_loop(first, members, step_body, 0, unroll=unroll)

    barrier = pltpu.get_barrier_semaphore()
    for distance in range(parts):

        def greet(step):
            row, col, _ = partner(distance, step)
            pl.semaphore_signal(barrier, inc=1, device_id=(row, col), device_id_type=MESH)

        each(1 if distance == 0 else 0, greet)

    def wait_bytes(ref, sem):
        pltpu.make_async_copy(ref, ref, sem).wait()

    def remote(source, target, send_sem, recv_sem, row, col):
        pltpu.make_async_remote_copy(
            src_ref=source,
            dst_ref=target,
            send_sem=send_sem,
            recv_sem=recv_sem,
            device_id=(row, col),
            device_id_type=MESH,
        ).start()

    row_at = pl.multiple_of(my_row * rows, rows)
    near_at = pl.multiple_of(my_near * rows, rows)
    col_at = pl.multiple_of(my_col * cols, cols)

    def panels(chunk, place):
        return pl.ds(chunk * wide + place * piece, piece)

    def first_targets(chunk):
        spot = pl.ds(chunk * piece, piece)
        a_to = recv_a.at[spot, pl.ds(near_at, rows), pl.ds(col_at, cols)]
        b_to = recv_b.at[spot, pl.ds(row_at, rows), pl.ds(col_at, cols)]
        return a_to, b_to

    def send_right(distance, chunk):
        _, b_to = first_targets(chunk)

        def right(step):
            row, col, place = partner(distance, step)
            source = send_ab0.at[1, panels(chunk, place)]
            remote(source, b_to, b_send_sem.at[distance], b_recv_sem.at[chunk], row, col)

        each(1 if distance == 0 else 0, right)

    def send_near_panels(chunk):
        a_to, b_to = first_targets(chunk)

        def left(step):
            row, col, place = partner(0, step)
            source = send_ab0.at[0, panels(chunk, place)]
            remote(source, a_to, a_send_sem, a_recv_sem.at[chunk], row, col)

        send_right(0, chunk)
        each(1, left)
        own = panels(chunk, my_place)
        pltpu.make_async_copy(send_ab0.at[0, own], a_to, a_recv_sem.at[chunk]).start()
        pltpu.make_async_copy(send_ab0.at[1, own], b_to, b_recv_sem.at[chunk]).start()

    def send_far_panels(chunk):
        for distance in range(parts - 1, 0, -1):
            send_right(distance, chunk)

    def send_second_panels(half, chunk):
        to = recv_ab.at[
            :, pl.ds(chunk * tiles, tiles), half, my_near, :, pl.ds(col_at, cols)
        ]

        def source_of(place):
            return send_ab1.at[:, half, pl.ds((chunk * members + place) * tiles, tiles)]

        def both(step):
            row, col, place = partner(0, step)
            remote(source_of(place), to, ab_send_sem, ab_recv_sem.at[chunk], row, col)

        each(1, both)
        pltpu.make_async_copy(source_of(my_place), to, ab_recv_sem.at[chunk]).start()

    def send_first_products(half, first, amount):
        lands = recv_x0.at[half, pl.ds(first, amount), pl.ds(my_place * tiles, tiles)]

        def source_of(row, col):
            along = pl.ds(pl.multiple_of(col * cols, cols), cols)
            return send_x0.at[
                half, pl.ds(first, amount), :, lax.rem(row, row_part), :, along
            ]

        def other(step):
            row, col, _ = partner(0, step)
            remote(source_of(row, col), lands, x0_send_sem, x0_recv_sem.at[half], row, col)

        each(1, other)
        own = source_of(my_row, my_col)
        pltpu.make_async_copy(own, lands, x0_recv_sem.at[half]).start()

    def send_second_products(chunk, near):
        spot = pl.ds(chunk * piece, piece)
        lands = recv_x1.at[my_group, panels(chunk, my_place)]

        def source_of(row, col):
            at = pl.ds(pl.multiple_of(row * rows, rows), rows)
            along = pl.ds(pl.multiple_of(col * cols, cols), cols)
            return send_x1.at[spot, at, along]

        def other(distance, step):
            row, col, _ = partner(distance, step)
            remote(
                source_of(row, col),
                lands,
                x1_send_sem.at[distance],
                x1_recv_sem.at[chunk],
                row,
                col,
            )

        if not near:
            for distance in range(parts - 1, 0, -1):
                each(0, functools.partial(other, distance))
            return
        each(1, functools.partial(other, 0))
        own = source_of(my_row, my_col)
        pltpu.make_async_copy(own, lands, x1_recv_sem.at[chunk]).start()

    def prepare(section):
        for block in range(4):
            span = slice(block * hidden, (block + 1) * hidden)
            turned = turn(held["panel_weight"][section, :, span])
            biases = splat(held["panel_bias"][pl.ds(section, 1), span], cols)
            for chunk in range(chunks):
                to = pl.ds((chunk * 4 + block) * wide, wide)
                weight_t[section, to, :] = turned[chunk * wide : (chunk + 1) * wide]
                bias_t[section, to, :] = biases[chunk * wide : (chunk + 1) * wide]

    def prepare_lines():
        gate_t[...] = turn(held["gate_weight"][0])
        output_t[...] = turn(held["output_weight"][0])
        names = (("gate_bias", 0), ("output_bias", 0), ("pair_gain", 1), ("pair_shift", 1))
        for at, (name, section) in enumerate(names):
            lines_t[2 + at] = splat(held[name][pl.ds(section, 1), :], cols)
        for section in range(2):
            for at, name in enumerate(("hidden_gain", "hidden_shift")):
                line = splat(held[name][pl.ds(section, 1), :], cols)
                affine_t[section, at] = jnp.broadcast_to(line[:, None, :], (hidden, sub, cols))

    def loop(first, steps, body):
        def step_body(r, carry):
            body(r)
            return carry

        lax.fori_loop(first, first + steps, step_body, 0, unroll=min(steps, 16))

    for at in urgent[:-1]:
        loads[at].wait()
    with jax.named_scope("prep0"):
        for at, name in enumerate(("pair_gain", "pair_shift")):
            lines_t[at] = splat(held[name][pl.ds(0, 1), :], cols)
        prepare(0)
    mask_load.wait()
    loads[urgent[-1]].wait()

    def first_norm(r):
        values = held["pair"][r].T
        pair_t[r] = values
        normed_ref[r] = normalize(values, 0, PAIR_EPSILON, lines_t[0], lines_t[1])

    with jax.named_scope("norm0"):
        loop(0, rows, first_norm)
    col_mask = held["mask"][pl.ds(my_col, 1), :].astype(jnp.float32)

    def project(section, chunk, height, first, r):
        span = pl.ds(chunk * 4 * wide, 4 * wide)
        features = lax.dot_general(
            weight_t[section, span, :],
            normed_ref[r],
            (((1,), (0,)), ((), ())),
            preferred_element_type=jnp.float32,
        )
        features = features + bias_t[section, span, :]
        mask = col_mask * mask_smem[my_row * rows + r].astype(jnp.float32)
        for which in range(2):
            at = 2 * which * wide
            panel = mask * jax.nn.sigmoid(features[at : at + wide])
            panel = panel * features[at + wide : at + 2 * wide]
            stage[which, pl.ds(r - first, wide, stride=height), :] = panel

    def make_first(chunk):
        loop(0, rows, functools.partial(project, 0, chunk, rows, 0))
        for which in range(2):
            send_ab0[which, pl.ds(chunk * wide, wide)] = (
                stage[which].astype(jnp.bfloat16).reshape(wide, rows, cols)
            )
        if chunk == 0:
            with jax.named_scope("barrier"):
                pl.semaphore_wait(barrier, devices - 1)
        send_far_panels(chunk)
        send_near_panels(chunk)

    def make_second(half, chunk):
        loop(half * sub, sub, functools.partial(project, 1, chunk, sub, half * sub))
        for which in range(2):
            made = stage[which, pl.ds(0, wide * sub), :].astype(jnp.bfloat16)
            send_ab1[which, half, pl.ds(chunk * members * tiles, members * tiles)] = (
                made.reshape(members * tiles, rows, cols)
            )
        send_second_panels(half, chunk)

    def first_gates(r):
        features = jnp.dot(gate_t[...], normed_ref[r], preferred_element_type=jnp.float32)
        gate[r] = jax.nn.sigmoid(features + lines_t[2])

    def second_gates(r):
        held["pair"][r] = pair_t[r].T
        features = lax.dot_general(
            normed_ref[r],
            held["gate_weight"][1],
            (((0,), (0,)), ((), ())),
            preferred_element_type=jnp.float32,
        )
        gate[r] = jax.nn.sigmoid(features + held["gate_bias"][pl.ds(1, 1), :])

    def multiply_first(chunk):
        spot = pl.ds(chunk * piece, piece)
        with jax.named_scope(f"waitab0_{chunk}"):
            wait_bytes(recv_a.at[spot], a_recv_sem.at[chunk])
            wait_bytes(recv_b.at[spot], b_recv_sem.at[chunk])
        for tile in range(tiles):
            products = []
            for h in range(halves):
                at = chunk * piece + tile * halves + h
                product = lax.dot_general(
                    recv_a[at],
                    recv_b[at],
                    (((1,), (1,)), ((), ())),
                    preferred_element_type=jnp.float32,
                )
                products.append(product.reshape(row_part, halves, sub, product.shape[1]))
            for half in range(halves):
                packed = jnp.concatenate([product[:, half] for product in products], axis=1)
                send_x0[half, chunk, tile] = packed.astype(jnp.bfloat16)

    def multiply_second(chunk):
        spot = pl.ds(chunk * tiles, tiles)
        with jax.named_scope(f"waitab1_{chunk}"):
            wait_bytes(recv_ab.at[:, spot], ab_recv_sem.at[chunk])
        for tile in range(tiles):
            sides = []
            for which in range(2):
                got = recv_ab[which, chunk * tiles + tile].astype(jnp.float32)
                got = got.reshape(halves * row_part, halves, sub, got.shape[-1])
                sides.append(got)
            for h in range(halves):
                left, right = (
                    side[:, h]
                    .reshape(row_part * rows, side.shape[-1])
                    .astype(jnp.bfloat16)
                    for side in sides
                )
                send_x1[chunk * piece + tile * halves + h] = lax.dot_general(
                    left,
                    right,
                    (((0,), (0,)), ((), ())),
                    preferred_element_type=jnp.float32,
                ).astype(jnp.bfloat16)
        send_second_products(chunk, False)

    strip = min(hidden, 16)

    def strips(half):
        for at in range(0, hidden, strip):
            spot = pl.ds(at * sub, strip * sub)
            yield at, spot, stage_x[half, spot, :].reshape(strip, sub, cols)

    def fill(half, at, values):
        stage_x[half, pl.ds(at * sub, values.shape[0] * sub), :] = values.reshape(-1, cols)
        return jnp.sum(values, axis=0)

    def normalize_hidden(section, half, summed):
        center = summed * (1.0 / hidden)
        spread = jnp.zeros((sub, cols), jnp.float32)
        for _, _, values in strips(half):
            offset = values - center
            spread = spread + jnp.sum(offset * offset, axis=0)
        scale = lax.rsqrt(spread * (1.0 / hidden) + HIDDEN_EPSILON)
        for at, spot, values in strips(half):
            normed = (values - center) * scale * affine_t[section, 0, pl.ds(at, strip)]
            normed = normed + affine_t[section, 1, pl.ds(at, strip)]
            stage_x[half, spot, :] = normed.reshape(strip * sub, cols)

    def finish_first(half):
        with jax.named_scope(f"waitx0_{half}"):
            wait_bytes(recv_x0.at[half], x0_recv_sem.at[half])
        with jax.named_scope(f"finish0_{half}"):
            summed = jnp.zeros((sub, cols), jnp.float32)
            for chunk in range(chunks):
                for at in range(0, members * tiles, strip // halves):
                    height = min(strip // halves, members * tiles)
                    got = recv_x0[half, chunk, pl.ds(at, height)].astype(jnp.float32)
                    got = got.reshape(height * halves, sub, cols)
                    summed = summed + fill(half, chunk * wide + at * halves, got)
            normalize_hidden(0, half, summed)

            def finish(r):
                normed = stage_x[half, pl.ds(r - half * sub, hidden, stride=sub), :]
                projected = jnp.dot(
                    output_t[...],
                    normed.astype(jnp.bfloat16),
                    preferred_element_type=jnp.float32,
                )
                updated = pair_t[r] + gate[r] * (projected + lines_t[3])
                pair_t[r] = updated
                normed_ref[r] = normalize(updated, 0, PAIR_EPSILON, lines_t[4], lines_t[5])

            loop(half * sub, sub, finish)

    for chunk in range(chunks):
        with jax.named_scope(f"make0_{chunk}"):
            make_first(chunk)
    for at in later:
        loads[at].wait()
    with jax.named_scope("gates0"):
        prepare_lines()
        loop(0, rows, first_gates)
        prepare(1)
    for chunk in range(chunks):
        with jax.named_scope(f"mult0_{chunk}"):
            multiply_first(chunk)
            if chunk == chunks - 2:
                send_first_products(0, 0, chunks - 1)
                for half in range(1, halves):
                    send_first_products(half, 0, chunks - 1)
            if chunk == chunks - 1:
                for half in range(halves):
                    send_first_products(half, chunk, 1)

    lead = min(LEAD, chunks)

    def produce(half, chunk):
        with jax.named_scope(f"make1_{half}_{chunk}"):
            make_second(half, chunk)

    early_chunks = min(1, chunks) if halves > 1 else 0
    for half in range(halves):
        finish_first(half)
        if half < halves - 1:
            for chunk in range(early_chunks):
                produce(half, chunk)
    for chunk in range(lead):
        for half in range(halves):
            if not (half < halves - 1 and chunk < early_chunks):
                produce(half, chunk)
    for chunk in range(chunks):
        with jax.named_scope(f"mult1_{chunk}"):
            multiply_second(chunk)
        if chunk + lead < chunks:
            for half in range(halves):
                produce(half, chunk + lead)
        if chunk >= 1:
            send_second_products(chunk - 1, True)
    for chunk in range(chunks - 1, chunks):
        send_second_products(chunk, True)
    with jax.named_scope("gates1"):
        loop(0, rows, second_gates)
    summed = [jnp.zeros((sub, cols), jnp.float32) for _ in range(halves)]
    for chunk in range(chunks):
        with jax.named_scope(f"waitx1_{chunk}"):
            wait_bytes(recv_x1.at[:, pl.ds(chunk * wide, wide)], x1_recv_sem.at[chunk])
        for at in range(chunk * wide, (chunk + 1) * wide, min(strip, wide)):
            height = min(strip, wide)
            got = recv_x1[0, pl.ds(at, height)].astype(jnp.float32)
            for other in range(1, parts):
                got = got + recv_x1[other, pl.ds(at, height)].astype(jnp.float32)
            got = got.reshape(height, halves, sub, cols)
            for half in range(halves):
                summed[half] = summed[half] + fill(half, at, got[:, half])

    with jax.named_scope("finish1"):
        for half in range(halves):
            normalize_hidden(1, half, summed[half])

            def finish(r):
                normed = stage_x[half, pl.ds(r - half * sub, hidden, stride=sub), :]
                projected = lax.dot_general(
                    normed.astype(jnp.bfloat16),
                    held["output_weight"][1],
                    (((0,), (0,)), ((), ())),
                    preferred_element_type=jnp.float32,
                )
                projected = projected + held["output_bias"][pl.ds(1, 1), :]
                out_ref[r] = held["pair"][r] + gate[r] * projected

            loop(half * sub, sub, finish)

    one = hidden - per_slot
    wait_bytes(send_ab0.at[0, pl.ds(0, one)], a_send_sem)
    wait_bytes(send_ab1.at[:, :, pl.ds(0, one // halves)], ab_send_sem)
    for distance in range(parts):
        amount = one if distance == 0 else hidden
        wait_bytes(send_ab0.at[1, pl.ds(0, amount)], b_send_sem.at[distance])
        wait_bytes(send_ab0.at[1, pl.ds(0, amount)], x1_send_sem.at[distance])
    wait_bytes(send_ab0.at[0, pl.ds(0, one)], x0_send_sem)


def local(row_total, col_total, pair_rep, residue_mask, *parameters):
    rows, cols, channels = pair_rep.shape
    hidden = parameters[2].shape[2] // 4
    parts = max(2, row_total * col_total // hidden)
    members = row_total * col_total // parts
    row_part = row_total // parts
    per_slot = hidden // members
    chunks = min(CHUNKS, per_slot)
    piece = per_slot // chunks
    halves = 2 if piece % 2 == 0 and rows % 16 == 0 else 1
    tiles = piece // halves
    sub = rows // halves
    wide = hidden // chunks
    total = row_total * rows
    part = total // parts
    sizes = (rows, cols, hidden, row_total, col_total, parts, chunks, halves)
    bf16, f32 = jnp.bfloat16, jnp.float32
    dma = pltpu.SemaphoreType.DMA
    arrays = (pair_rep, residue_mask.reshape(col_total, cols), *parameters)
    return pl.pallas_call(
        functools.partial(kernel, sizes),
        out_shape=pltpu.VMEM((rows, cols, channels), f32),
        in_specs=[pl.BlockSpec(memory_space=pltpu.HBM)] * (1 + len(arrays)),
        out_specs=pl.BlockSpec(memory_space=pltpu.VMEM),
        scratch_shapes=[pltpu.VMEM(array.shape, array.dtype) for array in arrays]
        + [
            pltpu.VMEM((2, 4 * hidden, channels), bf16),
            pltpu.VMEM((2, 4 * hidden, cols), f32),
            pltpu.VMEM((channels, channels), bf16),
            pltpu.VMEM((channels, hidden), bf16),
            pltpu.VMEM((6, channels, cols), f32),
            pltpu.VMEM((2, 2, hidden, sub, cols), f32),
            pltpu.VMEM((rows, channels, cols), bf16),
            pltpu.VMEM((2, wide * rows, cols), f32),
            pltpu.VMEM((halves, hidden * sub, cols), f32),
            pltpu.VMEM((rows, channels, cols), f32),
            pltpu.VMEM((rows, cols, channels), f32),
            pltpu.VMEM((2, hidden, rows, cols), bf16),
            pltpu.VMEM((2, halves, hidden // halves, rows, cols), bf16),
            pltpu.VMEM((per_slot, part, total), bf16),
            pltpu.VMEM((per_slot, total, total), bf16),
            pltpu.VMEM((2, per_slot // halves, halves, row_part, rows, total), bf16),
            pltpu.VMEM((halves, chunks, tiles, row_part, rows, total), bf16),
            pltpu.VMEM((per_slot, total, total), bf16),
            pltpu.VMEM((halves, chunks, members * tiles, rows, cols), bf16),
            pltpu.VMEM((parts, hidden, rows, cols), bf16),
            dma((len(arrays),)),
            dma(()),
            dma((chunks,)),
            dma((parts,)),
            dma((chunks,)),
            dma(()),
            dma((chunks,)),
            dma(()),
            dma((halves,)),
            dma((parts,)),
            dma((chunks,)),
            pltpu.SMEM(residue_mask.shape, residue_mask.dtype),
            dma(()),
        ],
        compiler_params=pltpu.CompilerParams(collective_id=0, has_side_effects=True),
    )(residue_mask, *arrays)


def solution(mesh):
    return jax.shard_map(
        functools.partial(local, mesh.shape["row"], mesh.shape["ch"]),
        mesh=mesh,
        in_specs=(P("row", "ch", None), P(), P(), P(), P(), P(), P(), P(), P(), P(), P(), P()),
        out_specs=P("row", "ch", None),
        check_vma=False,
    )
```

```python
import functools

import jax
import jax.numpy as jnp
from jax import lax
from jax.experimental import pallas as pl
from jax.experimental.pallas import tpu as pltpu
from jax.sharding import PartitionSpec as P

PAIR_EPSILON = 1e-05
HIDDEN_EPSILON = 1.0
MESH = pl.DeviceIdType.MESH
CHUNKS = 4
LEAD = 4
NAMES = (
    "pair",
    "mask",
    "pair_gain",
    "pair_shift",
    "panel_weight",
    "panel_bias",
    "gate_weight",
    "gate_bias",
    "hidden_gain",
    "hidden_shift",
    "output_weight",
    "output_bias",
)


def normalize(values, axis, epsilon, gain, shift):
    offset = values - jnp.mean(values, axis=axis, keepdims=True)
    spread = jnp.mean(offset * offset, axis=axis, keepdims=True)
    return (offset * lax.rsqrt(spread + epsilon) * gain + shift).astype(jnp.bfloat16)


def splat(line, cols):
    return jnp.broadcast_to(line, (cols, line.shape[1])).T


def turn(weight):
    return weight.astype(jnp.float32).T.astype(jnp.bfloat16)


def kernel(sizes, mask_hbm, *refs):
    rows, cols, hidden, row_total, col_total, parts, chunks, halves = sizes
    count = len(NAMES)
    sources = dict(zip(NAMES, refs[:count]))
    out_ref = refs[count]
    held = dict(zip(NAMES, refs[count + 1 : 2 * count + 1]))
    (
        weight_t,
        bias_t,
        gate_t,
        output_t,
        lines_t,
        affine_t,
        normed_ref,
        stage,
        stage_x,
        pair_t,
        gate,
        send_ab0,
        send_ab1,
        recv_a,
        recv_b,
        recv_ab,
        send_x0,
        send_x1,
        recv_x0,
        recv_x1,
        load_sem,
        a_send_sem,
        a_recv_sem,
        b_send_sem,
        b_recv_sem,
        ab_send_sem,
        ab_recv_sem,
        x0_send_sem,
        x0_recv_sem,
        x1_send_sem,
        x1_recv_sem,
        mask_smem,
        mask_sem,
    ) = refs[2 * count + 1 :]
    devices = row_total * col_total
    row_part = row_total // parts
    members = row_part * col_total
    per_slot = hidden // members
    piece = per_slot // chunks
    wide = hidden // chunks
    sub = rows // halves
    tiles = piece // halves
    my_row = lax.axis_index("row")
    my_col = lax.axis_index("ch")
    my_group = my_row // row_part
    my_near = lax.rem(my_row, row_part)
    my_place = my_near * col_total + my_col

    loads = [
        pltpu.make_async_copy(sources[name], held[name], load_sem.at[at])
        for at, name in enumerate(NAMES)
    ]
    order = ("panel_weight", "pair_gain", "pair_shift", "panel_bias", "mask", "pair")
    urgent = [NAMES.index(name) for name in order]
    later = [at for at in range(count) if at not in urgent]
    mask_load = pltpu.make_async_copy(mask_hbm, mask_smem, mask_sem)
    for at in urgent:
        loads[at].start()
    mask_load.start()
    for at in later:
        loads[at].start()

    def partner(distance, step):
        group = lax.rem(my_group + distance, parts)
        if members & (members - 1):
            place = lax.rem(my_place + step, members)
        else:
            reach = members - step if distance == 0 else members - 1 - step
            place = my_place ^ reach
        return group * row_part + place // col_total, lax.rem(place, col_total), place

    def each(first, body):
        def step_body(step, carry):
            body(step)
            return carry

        steps = members - first
        unroll = max(d for d in (1, 4, 5) if steps % d == 0)
        lax.fori_loop(first, members, step_body, 0, unroll=unroll)

    barrier = pltpu.get_barrier_semaphore()
    for distance in range(parts):

        def greet(step):
            row, col, _ = partner(distance, step)
            pl.semaphore_signal(barrier, inc=1, device_id=(row, col), device_id_type=MESH)

        each(1 if distance == 0 else 0, greet)

    def wait_bytes(ref, sem):
        pltpu.make_async_copy(ref, ref, sem).wait()

    def remote(source, target, send_sem, recv_sem, row, col):
        pltpu.make_async_remote_copy(
            src_ref=source,
            dst_ref=target,
            send_sem=send_sem,
            recv_sem=recv_sem,
            device_id=(row, col),
            device_id_type=MESH,
        ).start()

    row_at = pl.multiple_of(my_row * rows, rows)
    near_at = pl.multiple_of(my_near * rows, rows)
    col_at = pl.multiple_of(my_col * cols, cols)

    def panels(chunk, place):
        return pl.ds(chunk * wide + place * piece, piece)

    def first_targets(chunk):
        spot = pl.ds(chunk * piece, piece)
        a_to = recv_a.at[spot, pl.ds(near_at, rows), pl.ds(col_at, cols)]
        b_to = recv_b.at[spot, pl.ds(row_at, rows), pl.ds(col_at, cols)]
        return a_to, b_to

    def send_right(distance, chunk):
        _, b_to = first_targets(chunk)

        def right(step):
            row, col, place = partner(distance, step)
            source = send_ab0.at[1, panels(chunk, place)]
            remote(source, b_to, b_send_sem.at[distance], b_recv_sem.at[chunk], row, col)

        each(1 if distance == 0 else 0, right)

    def send_near_panels(chunk):
        a_to, b_to = first_targets(chunk)

        def left(step):
            row, col, place = partner(0, step)
            source = send_ab0.at[0, panels(chunk, place)]
            remote(source, a_to, a_send_sem, a_recv_sem.at[chunk], row, col)

        send_right(0, chunk)
        each(1, left)
        own = panels(chunk, my_place)
        pltpu.make_async_copy(send_ab0.at[0, own], a_to, a_recv_sem.at[chunk]).start()
        pltpu.make_async_copy(send_ab0.at[1, own], b_to, b_recv_sem.at[chunk]).start()

    def send_far_panels(chunk):
        for distance in range(parts - 1, 0, -1):
            send_right(distance, chunk)

    def send_second_panels(half, chunk):
        to = recv_ab.at[
            :, pl.ds(chunk * tiles, tiles), half, my_near, :, pl.ds(col_at, cols)
        ]

        def source_of(place):
            return send_ab1.at[:, half, pl.ds((chunk * members + place) * tiles, tiles)]

        def both(step):
            row, col, place = partner(0, step)
            remote(source_of(place), to, ab_send_sem, ab_recv_sem.at[chunk], row, col)

        each(1, both)
        pltpu.make_async_copy(source_of(my_place), to, ab_recv_sem.at[chunk]).start()

    def send_first_products(half, first, amount):
        lands = recv_x0.at[half, pl.ds(first, amount), pl.ds(my_place * tiles, tiles)]

        def source_of(row, col):
            along = pl.ds(pl.multiple_of(col * cols, cols), cols)
            return send_x0.at[
                half, pl.ds(first, amount), :, lax.rem(row, row_part), :, along
            ]

        def other(step):
            row, col, _ = partner(0, step)
            remote(source_of(row, col), lands, x0_send_sem, x0_recv_sem.at[half], row, col)

        each(1, other)
        own = source_of(my_row, my_col)
        pltpu.make_async_copy(own, lands, x0_recv_sem.at[half]).start()

    def send_second_products(chunk, near):
        spot = pl.ds(chunk * piece, piece)
        lands = recv_x1.at[my_group, panels(chunk, my_place)]

        def source_of(row, col):
            at = pl.ds(pl.multiple_of(row * rows, rows), rows)
            along = pl.ds(pl.multiple_of(col * cols, cols), cols)
            return send_x1.at[spot, at, along]

        def other(distance, step):
            row, col, _ = partner(distance, step)
            remote(
                source_of(row, col),
                lands,
                x1_send_sem.at[distance],
                x1_recv_sem.at[chunk],
                row,
                col,
            )

        if not near:
            for distance in range(parts - 1, 0, -1):
                each(0, functools.partial(other, distance))
            return
        each(1, functools.partial(other, 0))
        own = source_of(my_row, my_col)
        pltpu.make_async_copy(own, lands, x1_recv_sem.at[chunk]).start()

    def prepare(section):
        for block in range(4):
            span = slice(block * hidden, (block + 1) * hidden)
            turned = turn(held["panel_weight"][section, :, span])
            biases = splat(held["panel_bias"][pl.ds(section, 1), span], cols)
            for chunk in range(chunks):
                to = pl.ds((chunk * 4 + block) * wide, wide)
                weight_t[section, to, :] = turned[chunk * wide : (chunk + 1) * wide]
                bias_t[section, to, :] = biases[chunk * wide : (chunk + 1) * wide]

    def prepare_lines():
        gate_t[...] = turn(held["gate_weight"][0])
        output_t[...] = turn(held["output_weight"][0])
        names = (("gate_bias", 0), ("output_bias", 0), ("pair_gain", 1), ("pair_shift", 1))
        for at, (name, section) in enumerate(names):
            lines_t[2 + at] = splat(held[name][pl.ds(section, 1), :], cols)
        for section in range(2):
            for at, name in enumerate(("hidden_gain", "hidden_shift")):
                line = splat(held[name][pl.ds(section, 1), :], cols)
                affine_t[section, at] = jnp.broadcast_to(line[:, None, :], (hidden, sub, cols))

    def loop(first, steps, body):
        def step_body(r, carry):
            body(r)
            return carry

        lax.fori_loop(first, first + steps, step_body, 0, unroll=min(steps, 16))

    for at in urgent[:-1]:
        loads[at].wait()
    with jax.named_scope("prep0"):
        for at, name in enumerate(("pair_gain", "pair_shift")):
            lines_t[at] = splat(held[name][pl.ds(0, 1), :], cols)
        prepare(0)
    mask_load.wait()
    loads[urgent[-1]].wait()

    def first_norm(r):
        values = held["pair"][r].T
        pair_t[r] = values
        normed_ref[r] = normalize(values, 0, PAIR_EPSILON, lines_t[0], lines_t[1])

    with jax.named_scope("norm0"):
        loop(0, rows, first_norm)
    col_mask = held["mask"][pl.ds(my_col, 1), :].astype(jnp.float32)

    def project(section, chunk, height, first, r, sides=(0, 1)):
        span = pl.ds((chunk * 4 + 2 * sides[0]) * wide, 2 * len(sides) * wide)
        features = lax.dot_general(
            weight_t[section, span, :],
            normed_ref[r],
            (((1,), (0,)), ((), ())),
            preferred_element_type=jnp.float32,
        )
        features = features + bias_t[section, span, :]
        mask = col_mask * mask_smem[my_row * rows + r].astype(jnp.float32)
        for which in sides:
            at = 2 * (which - sides[0]) * wide
            panel = mask * jax.nn.sigmoid(features[at : at + wide])
            panel = panel * features[at + wide : at + 2 * wide]
            stage[which, pl.ds(r - first, wide, stride=height), :] = panel

    def make_first(chunk):
        for sides in ((1,), (0,)) if chunk == 0 else ((0, 1),):
            loop(0, rows, functools.partial(project, 0, chunk, rows, 0, sides=sides))
            for which in sides:
                send_ab0[which, pl.ds(chunk * wide, wide)] = (
                    stage[which].astype(jnp.bfloat16).reshape(wide, rows, cols)
                )
            if sides == (1,):
                with jax.named_scope("barrier"):
                    pl.semaphore_wait(barrier, devices - 1)
            if 1 in sides:
                send_far_panels(chunk)
        send_near_panels(chunk)

    def make_second(half, chunk):
        loop(half * sub, sub, functools.partial(project, 1, chunk, sub, half * sub))
        for which in range(2):
            made = stage[which, pl.ds(0, wide * sub), :].astype(jnp.bfloat16)
            send_ab1[which, half, pl.ds(chunk * members * tiles, members * tiles)] = (
                made.reshape(members * tiles, rows, cols)
            )
        send_second_panels(half, chunk)

    def first_gates(r):
        features = jnp.dot(gate_t[...], normed_ref[r], preferred_element_type=jnp.float32)
        gate[r] = jax.nn.sigmoid(features + lines_t[2])

    def second_gates(r):
        features = lax.dot_general(
            normed_ref[r],
            held["gate_weight"][1],
            (((0,), (0,)), ((), ())),
            preferred_element_type=jnp.float32,
        )
        value = jax.nn.sigmoid(features + held["gate_bias"][pl.ds(1, 1), :])
        gate[r] = value
        held["pair"][r] = pair_t[r].T + value * held["output_bias"][pl.ds(1, 1), :]

    def multiply_first(chunk):
        spot = pl.ds(chunk * piece, piece)
        with jax.named_scope(f"waitab0_{chunk}"):
            wait_bytes(recv_a.at[spot], a_recv_sem.at[chunk])
            wait_bytes(recv_b.at[spot], b_recv_sem.at[chunk])
        for tile in range(tiles):
            products = []
            for h in range(halves):
                at = chunk * piece + tile * halves + h
                product = lax.dot_general(
                    recv_a[at],
                    recv_b[at],
                    (((1,), (1,)), ((), ())),
                    preferred_element_type=jnp.float32,
                )
                products.append(product.reshape(row_part, halves, sub, product.shape[1]))
            for half in range(halves):
                packed = jnp.concatenate([product[:, half] for product in products], axis=1)
                send_x0[half, chunk, tile] = packed.astype(jnp.bfloat16)

    def multiply_second(chunk):
        spot = pl.ds(chunk * tiles, tiles)
        with jax.named_scope(f"waitab1_{chunk}"):
            wait_bytes(recv_ab.at[:, spot], ab_recv_sem.at[chunk])
        for tile in range(tiles):
            sides = []
            for which in range(2):
                got = recv_ab[which, chunk * tiles + tile].astype(jnp.float32)
                got = got.reshape(halves * row_part, halves, sub, got.shape[-1])
                sides.append(got)
            for h in range(halves):
                left, right = (
                    side[:, h]
                    .reshape(row_part * rows, side.shape[-1])
                    .astype(jnp.bfloat16)
                    for side in sides
                )
                send_x1[chunk * piece + tile * halves + h] = lax.dot_general(
                    left,
                    right,
                    (((0,), (0,)), ((), ())),
                    preferred_element_type=jnp.float32,
                ).astype(jnp.bfloat16)
        send_second_products(chunk, False)

    strip = min(hidden, 16)

    def strips(half):
        for at in range(0, hidden, strip):
            spot = pl.ds(at * sub, strip * sub)
            yield at, spot, stage_x[half, spot, :].reshape(strip, sub, cols)

    def fill(half, at, values):
        stage_x[half, pl.ds(at * sub, values.shape[0] * sub), :] = values.reshape(-1, cols)
        return jnp.sum(values, axis=0)

    def normalize_hidden(section, half, summed):
        center = summed * (1.0 / hidden)
        spread = jnp.zeros((sub, cols), jnp.float32)
        for _, _, values in strips(half):
            offset = values - center
            spread = spread + jnp.sum(offset * offset, axis=0)
        scale = lax.rsqrt(spread * (1.0 / hidden) + HIDDEN_EPSILON)
        for at, spot, values in strips(half):
            normed = (values - center) * scale * affine_t[section, 0, pl.ds(at, strip)]
            normed = normed + affine_t[section, 1, pl.ds(at, strip)]
            stage_x[half, spot, :] = normed.reshape(strip * sub, cols)

    def finish_first(half):
        with jax.named_scope(f"waitx0_{half}"):
            wait_bytes(recv_x0.at[half], x0_recv_sem.at[half])
        with jax.named_scope(f"finish0_{half}"):
            summed = jnp.zeros((sub, cols), jnp.float32)
            for chunk in range(chunks):
                for at in range(0, members * tiles, strip // halves):
                    height = min(strip // halves, members * tiles)
                    got = recv_x0[half, chunk, pl.ds(at, height)].astype(jnp.float32)
                    got = got.reshape(height * halves, sub, cols)
                    summed = summed + fill(half, chunk * wide + at * halves, got)
            normalize_hidden(0, half, summed)

            def finish(r):
                normed = stage_x[half, pl.ds(r - half * sub, hidden, stride=sub), :]
                projected = jnp.dot(
                    output_t[...],
                    normed.astype(jnp.bfloat16),
                    preferred_element_type=jnp.float32,
                )
                updated = pair_t[r] + gate[r] * (projected + lines_t[3])
                pair_t[r] = updated
                normed_ref[r] = normalize(updated, 0, PAIR_EPSILON, lines_t[4], lines_t[5])

            loop(half * sub, sub, finish)

    for chunk in range(chunks):
        with jax.named_scope(f"make0_{chunk}"):
            make_first(chunk)
    for at in later:
        loads[at].wait()
    with jax.named_scope("gates0"):
        prepare_lines()
        loop(0, rows, first_gates)
        prepare(1)
    for chunk in range(chunks):
        with jax.named_scope(f"mult0_{chunk}"):
            multiply_first(chunk)
            if chunk == chunks - 2:
                send_first_products(0, 0, chunks - 1)
                for half in range(1, halves):
                    send_first_products(half, 0, chunks - 1)
            if chunk == chunks - 1:
                for half in range(halves):
                    send_first_products(half, chunk, 1)

    lead = min(LEAD, chunks)

    def produce(half, chunk):
        with jax.named_scope(f"make1_{half}_{chunk}"):
            make_second(half, chunk)

    early_chunks = min(1, chunks) if halves > 1 else 0
    for half in range(halves):
        finish_first(half)
        if half < halves - 1:
            for chunk in range(early_chunks):
                produce(half, chunk)
    for chunk in range(lead):
        for half in range(halves):
            if not (half < halves - 1 and chunk < early_chunks):
                produce(half, chunk)
    for chunk in range(chunks):
        with jax.named_scope(f"mult1_{chunk}"):
            multiply_second(chunk)
        if chunk + lead < chunks:
            for half in range(halves):
                produce(half, chunk + lead)
        if chunk >= 1:
            send_second_products(chunk - 1, True)
    for chunk in range(chunks - 1, chunks):
        send_second_products(chunk, True)
    with jax.named_scope("gates1"):
        loop(0, rows, second_gates)
    summed = [jnp.zeros((sub, cols), jnp.float32) for _ in range(halves)]
    for chunk in range(chunks):
        with jax.named_scope(f"waitx1_{chunk}"):
            wait_bytes(recv_x1.at[:, pl.ds(chunk * wide, wide)], x1_recv_sem.at[chunk])
        for at in range(chunk * wide, (chunk + 1) * wide, min(strip, wide)):
            height = min(strip, wide)
            got = recv_x1[0, pl.ds(at, height)].astype(jnp.float32)
            for other in range(1, parts):
                got = got + recv_x1[other, pl.ds(at, height)].astype(jnp.float32)
            got = got.reshape(height, halves, sub, cols)
            for half in range(halves):
                summed[half] = summed[half] + fill(half, at, got[:, half])

    with jax.named_scope("finish1"):
        for half in range(halves):
            normalize_hidden(1, half, summed[half])

            def finish(r):
                normed = stage_x[half, pl.ds(r - half * sub, hidden, stride=sub), :]
                projected = lax.dot_general(
                    normed.astype(jnp.bfloat16),
                    held["output_weight"][1],
                    (((0,), (0,)), ((), ())),
                    preferred_element_type=jnp.float32,
                )
                out_ref[r] = held["pair"][r] + gate[r] * projected

            loop(half * sub, sub, finish)

    one = hidden - per_slot
    wait_bytes(send_ab0.at[0, pl.ds(0, one)], a_send_sem)
    wait_bytes(send_ab1.at[:, :, pl.ds(0, one // halves)], ab_send_sem)
    for distance in range(parts):
        amount = one if distance == 0 else hidden
        wait_bytes(send_ab0.at[1, pl.ds(0, amount)], b_send_sem.at[distance])
        wait_bytes(send_ab0.at[1, pl.ds(0, amount)], x1_send_sem.at[distance])
    wait_bytes(send_ab0.at[0, pl.ds(0, one)], x0_send_sem)


def local(row_total, col_total, pair_rep, residue_mask, *parameters):
    rows, cols, channels = pair_rep.shape
    hidden = parameters[2].shape[2] // 4
    parts = max(2, row_total * col_total // hidden)
    members = row_total * col_total // parts
    row_part = row_total // parts
    per_slot = hidden // members
    chunks = min(CHUNKS, per_slot)
    piece = per_slot // chunks
    halves = 2 if piece % 2 == 0 and rows % 16 == 0 else 1
    tiles = piece // halves
    sub = rows // halves
    wide = hidden // chunks
    total = row_total * rows
    part = total // parts
    sizes = (rows, cols, hidden, row_total, col_total, parts, chunks, halves)
    bf16, f32 = jnp.bfloat16, jnp.float32
    dma = pltpu.SemaphoreType.DMA
    arrays = (pair_rep, residue_mask.reshape(col_total, cols), *parameters)
    return pl.pallas_call(
        functools.partial(kernel, sizes),
        out_shape=pltpu.VMEM((rows, cols, channels), f32),
        in_specs=[pl.BlockSpec(memory_space=pltpu.HBM)] * (1 + len(arrays)),
        out_specs=pl.BlockSpec(memory_space=pltpu.VMEM),
        scratch_shapes=[pltpu.VMEM(array.shape, array.dtype) for array in arrays]
        + [
            pltpu.VMEM((2, 4 * hidden, channels), bf16),
            pltpu.VMEM((2, 4 * hidden, cols), f32),
            pltpu.VMEM((channels, channels), bf16),
            pltpu.VMEM((channels, hidden), bf16),
            pltpu.VMEM((6, channels, cols), f32),
            pltpu.VMEM((2, 2, hidden, sub, cols), f32),
            pltpu.VMEM((rows, channels, cols), bf16),
            pltpu.VMEM((2, wide * rows, cols), f32),
            pltpu.VMEM((halves, hidden * sub, cols), f32),
            pltpu.VMEM((rows, channels, cols), f32),
            pltpu.VMEM((rows, cols, channels), f32),
            pltpu.VMEM((2, hidden, rows, cols), bf16),
            pltpu.VMEM((2, halves, hidden // halves, rows, cols), bf16),
            pltpu.VMEM((per_slot, part, total), bf16),
            pltpu.VMEM((per_slot, total, total), bf16),
            pltpu.VMEM((2, per_slot // halves, halves, row_part, rows, total), bf16),
            pltpu.VMEM((halves, chunks, tiles, row_part, rows, total), bf16),
            pltpu.VMEM((per_slot, total, total), bf16),
            pltpu.VMEM((halves, chunks, members * tiles, rows, cols), bf16),
            pltpu.VMEM((parts, hidden, rows, cols), bf16),
            dma((len(arrays),)),
            dma(()),
            dma((chunks,)),
            dma((parts,)),
            dma((chunks,)),
            dma(()),
            dma((chunks,)),
            dma(()),
            dma((halves,)),
            dma((parts,)),
            dma((chunks,)),
            pltpu.SMEM(residue_mask.shape, residue_mask.dtype),
            dma(()),
        ],
        compiler_params=pltpu.CompilerParams(collective_id=0, has_side_effects=True),
    )(residue_mask, *arrays)


def solution(mesh):
    return jax.shard_map(
        functools.partial(local, mesh.shape["row"], mesh.shape["ch"]),
        mesh=mesh,
        in_specs=(P("row", "ch", None), P(), P(), P(), P(), P(), P(), P(), P(), P(), P(), P()),
        out_specs=P("row", "ch", None),
        check_vma=False,
    )
```

```python
import functools

import jax
import jax.numpy as jnp
from jax import lax
from jax.experimental import pallas as pl
from jax.experimental.pallas import tpu as pltpu
from jax.sharding import PartitionSpec as P

PAIR_EPSILON = 1e-05
HIDDEN_EPSILON = 1.0
MESH = pl.DeviceIdType.MESH
CHUNKS = 4
LEAD = 4
NAMES = (
    "pair",
    "mask",
    "pair_gain",
    "pair_shift",
    "panel_weight",
    "panel_bias",
    "gate_weight",
    "gate_bias",
    "hidden_gain",
    "hidden_shift",
    "output_weight",
    "output_bias",
)


def normalize(values, axis, epsilon, gain, shift):
    offset = values - jnp.mean(values, axis=axis, keepdims=True)
    spread = jnp.mean(offset * offset, axis=axis, keepdims=True)
    return (offset * lax.rsqrt(spread + epsilon) * gain + shift).astype(jnp.bfloat16)


def splat(line, cols):
    return jnp.broadcast_to(line, (cols, line.shape[1])).T


def turn(weight):
    return weight.astype(jnp.float32).T.astype(jnp.bfloat16)


def kernel(sizes, mask_hbm, *refs):
    rows, cols, hidden, row_total, col_total, parts, chunks, halves = sizes
    count = len(NAMES)
    sources = dict(zip(NAMES, refs[:count]))
    out_ref = refs[count]
    held = dict(zip(NAMES, refs[count + 1 : 2 * count + 1]))
    (
        weight_t,
        bias_t,
        gate_t,
        output_t,
        lines_t,
        affine_t,
        normed_ref,
        stage,
        stage_x,
        pair_t,
        gate,
        send_ab0,
        send_ab1,
        recv_a,
        recv_b,
        recv_ab,
        send_x0,
        send_x1,
        recv_x0,
        recv_x1,
        load_sem,
        a_send_sem,
        a_recv_sem,
        b_send_sem,
        b_recv_sem,
        ab_send_sem,
        ab_recv_sem,
        x0_send_sem,
        x0_recv_sem,
        x1_send_sem,
        x1_recv_sem,
        mask_smem,
        mask_sem,
    ) = refs[2 * count + 1 :]
    devices = row_total * col_total
    row_part = row_total // parts
    members = row_part * col_total
    per_slot = hidden // members
    piece = per_slot // chunks
    wide = hidden // chunks
    sub = rows // halves
    tiles = piece // halves
    my_row = lax.axis_index("row")
    my_col = lax.axis_index("ch")
    my_group = my_row // row_part
    my_near = lax.rem(my_row, row_part)
    my_place = my_near * col_total + my_col

    loads = [
        pltpu.make_async_copy(sources[name], held[name], load_sem.at[at])
        for at, name in enumerate(NAMES)
    ]
    order = ("panel_weight", "pair_gain", "pair_shift", "panel_bias", "mask", "pair")
    urgent = [NAMES.index(name) for name in order]
    later = [at for at in range(count) if at not in urgent]
    mask_load = pltpu.make_async_copy(mask_hbm, mask_smem, mask_sem)
    for at in urgent:
        loads[at].start()
    mask_load.start()
    for at in later:
        loads[at].start()

    def partner(distance, step):
        group = lax.rem(my_group + distance, parts)
        if members & (members - 1):
            place = lax.rem(my_place + step, members)
        else:
            reach = members - step if distance == 0 else members - 1 - step
            place = my_place ^ reach
        return group * row_part + place // col_total, lax.rem(place, col_total), place

    def each(first, body):
        def step_body(step, carry):
            body(step)
            return carry

        steps = members - first
        unroll = max(d for d in (1, 4, 5) if steps % d == 0)
        lax.fori_loop(first, members, step_body, 0, unroll=unroll)

    barrier = pltpu.get_barrier_semaphore()
    for distance in range(parts):

        def greet(step):
            row, col, _ = partner(distance, step)
            pl.semaphore_signal(barrier, inc=1, device_id=(row, col), device_id_type=MESH)

        each(1 if distance == 0 else 0, greet)

    def wait_bytes(ref, sem):
        pltpu.make_async_copy(ref, ref, sem).wait()

    def remote(source, target, send_sem, recv_sem, row, col):
        pltpu.make_async_remote_copy(
            src_ref=source,
            dst_ref=target,
            send_sem=send_sem,
            recv_sem=recv_sem,
            device_id=(row, col),
            device_id_type=MESH,
        ).start()

    row_at = pl.multiple_of(my_row * rows, rows)
    near_at = pl.multiple_of(my_near * rows, rows)
    col_at = pl.multiple_of(my_col * cols, cols)

    def panels(chunk, place):
        return pl.ds(chunk * wide + place * piece, piece)

    def first_targets(chunk):
        spot = pl.ds(chunk * piece, piece)
        a_to = recv_a.at[spot, pl.ds(near_at, rows), pl.ds(col_at, cols)]
        b_to = recv_b.at[spot, pl.ds(row_at, rows), pl.ds(col_at, cols)]
        return a_to, b_to

    def send_right(distance, chunk):
        _, b_to = first_targets(chunk)

        def right(step):
            row, col, place = partner(distance, step)
            source = send_ab0.at[1, panels(chunk, place)]
            remote(source, b_to, b_send_sem.at[distance], b_recv_sem.at[chunk], row, col)

        each(1 if distance == 0 else 0, right)

    def send_near_panels(chunk):
        a_to, b_to = first_targets(chunk)

        def left(step):
            row, col, place = partner(0, step)
            source = send_ab0.at[0, panels(chunk, place)]
            remote(source, a_to, a_send_sem, a_recv_sem.at[chunk], row, col)

        send_right(0, chunk)
        each(1, left)
        own = panels(chunk, my_place)
        pltpu.make_async_copy(send_ab0.at[0, own], a_to, a_recv_sem.at[chunk]).start()
        pltpu.make_async_copy(send_ab0.at[1, own], b_to, b_recv_sem.at[chunk]).start()

    def send_far_panels(chunk):
        for distance in range(parts - 1, 0, -1):
            send_right(distance, chunk)

    def send_second_panels(half, chunk):
        to = recv_ab.at[
            :, pl.ds(chunk * tiles, tiles), half, my_near, :, pl.ds(col_at, cols)
        ]

        def source_of(place):
            return send_ab1.at[:, half, pl.ds((chunk * members + place) * tiles, tiles)]

        def both(step):
            row, col, place = partner(0, step)
            remote(source_of(place), to, ab_send_sem, ab_recv_sem.at[chunk], row, col)

        each(1, both)
        pltpu.make_async_copy(source_of(my_place), to, ab_recv_sem.at[chunk]).start()

    def send_first_products(half, first, amount):
        lands = recv_x0.at[half, pl.ds(first, amount), pl.ds(my_place * tiles, tiles)]

        def source_of(row, col):
            along = pl.ds(pl.multiple_of(col * cols, cols), cols)
            return send_x0.at[
                half, pl.ds(first, amount), :, lax.rem(row, row_part), :, along
            ]

        def other(step):
            row, col, _ = partner(0, step)
            remote(source_of(row, col), lands, x0_send_sem, x0_recv_sem.at[half], row, col)

        each(1, other)
        own = source_of(my_row, my_col)
        pltpu.make_async_copy(own, lands, x0_recv_sem.at[half]).start()

    def send_second_products(chunk, near):
        spot = pl.ds(chunk * piece, piece)
        lands = recv_x1.at[my_group, panels(chunk, my_place)]

        def source_of(row, col):
            at = pl.ds(pl.multiple_of(row * rows, rows), rows)
            along = pl.ds(pl.multiple_of(col * cols, cols), cols)
            return send_x1.at[spot, at, along]

        def other(distance, step):
            row, col, _ = partner(distance, step)
            remote(
                source_of(row, col),
                lands,
                x1_send_sem.at[distance],
                x1_recv_sem.at[chunk],
                row,
                col,
            )

        if not near:
            for distance in range(parts - 1, 0, -1):
                each(0, functools.partial(other, distance))
            return
        each(1, functools.partial(other, 0))
        own = source_of(my_row, my_col)
        pltpu.make_async_copy(own, lands, x1_recv_sem.at[chunk]).start()

    def prepare(section):
        for block in range(4):
            span = slice(block * hidden, (block + 1) * hidden)
            turned = turn(held["panel_weight"][section, :, span])
            biases = splat(held["panel_bias"][pl.ds(section, 1), span], cols)
            for chunk in range(chunks):
                to = pl.ds((chunk * 4 + block) * wide, wide)
                weight_t[section, to, :] = turned[chunk * wide : (chunk + 1) * wide]
                bias_t[section, to, :] = biases[chunk * wide : (chunk + 1) * wide]

    def prepare_lines():
        gate_t[...] = turn(held["gate_weight"][0])
        output_t[...] = turn(held["output_weight"][0])
        names = (("gate_bias", 0), ("output_bias", 0), ("pair_gain", 1), ("pair_shift", 1))
        for at, (name, section) in enumerate(names):
            lines_t[2 + at] = splat(held[name][pl.ds(section, 1), :], cols)
        for section in range(2):
            for at, name in enumerate(("hidden_gain", "hidden_shift")):
                line = splat(held[name][pl.ds(section, 1), :], cols)
                affine_t[section, at] = jnp.broadcast_to(line[:, None, :], (hidden, sub, cols))

    def loop(first, steps, body):
        def step_body(r, carry):
            body(r)
            return carry

        lax.fori_loop(first, first + steps, step_body, 0, unroll=min(steps, 16))

    for at in urgent[:-1]:
        loads[at].wait()
    with jax.named_scope("prep0"):
        for at, name in enumerate(("pair_gain", "pair_shift")):
            lines_t[at] = splat(held[name][pl.ds(0, 1), :], cols)
        prepare(0)
    mask_load.wait()
    loads[urgent[-1]].wait()

    def first_norm(r):
        values = held["pair"][r].T
        pair_t[r] = values
        normed_ref[r] = normalize(values, 0, PAIR_EPSILON, lines_t[0], lines_t[1])

    with jax.named_scope("norm0"):
        loop(0, rows, first_norm)
    col_mask = held["mask"][pl.ds(my_col, 1), :].astype(jnp.float32)

    def project(section, chunk, height, first, r, sides=(0, 1)):
        span = pl.ds((chunk * 4 + 2 * sides[0]) * wide, 2 * len(sides) * wide)
        features = lax.dot_general(
            weight_t[section, span, :],
            normed_ref[r],
            (((1,), (0,)), ((), ())),
            preferred_element_type=jnp.float32,
        )
        features = features + bias_t[section, span, :]
        mask = col_mask * mask_smem[my_row * rows + r].astype(jnp.float32)
        for which in sides:
            at = 2 * (which - sides[0]) * wide
            panel = mask * jax.nn.sigmoid(features[at : at + wide])
            panel = panel * features[at + wide : at + 2 * wide]
            stage[which, pl.ds(r - first, wide, stride=height), :] = panel

    def make_first(chunk):
        for sides in ((1,), (0,)) if chunk == 0 else ((0, 1),):
            loop(0, rows, functools.partial(project, 0, chunk, rows, 0, sides=sides))
            for which in sides:
                send_ab0[which, pl.ds(chunk * wide, wide)] = (
                    stage[which].astype(jnp.bfloat16).reshape(wide, rows, cols)
                )
            if sides == (1,):
                with jax.named_scope("barrier"):
                    pl.semaphore_wait(barrier, devices - 1)
            if 1 in sides:
                send_far_panels(chunk)
        send_near_panels(chunk)

    def make_second(half, chunk):
        loop(half * sub, sub, functools.partial(project, 1, chunk, sub, half * sub))
        for which in range(2):
            made = stage[which, pl.ds(0, wide * sub), :].astype(jnp.bfloat16)
            send_ab1[which, half, pl.ds(chunk * members * tiles, members * tiles)] = (
                made.reshape(members * tiles, rows, cols)
            )
        send_second_panels(half, chunk)

    def first_gates(r):
        features = jnp.dot(gate_t[...], normed_ref[r], preferred_element_type=jnp.float32)
        gate[r] = jax.nn.sigmoid(features + lines_t[2])

    def second_gates(r):
        features = lax.dot_general(
            normed_ref[r],
            held["gate_weight"][1],
            (((0,), (0,)), ((), ())),
            preferred_element_type=jnp.float32,
        )
        value = jax.nn.sigmoid(features + held["gate_bias"][pl.ds(1, 1), :])
        gate[r] = value
        held["pair"][r] = pair_t[r].T + value * held["output_bias"][pl.ds(1, 1), :]

    def multiply_first(chunk):
        spot = pl.ds(chunk * piece, piece)
        with jax.named_scope(f"waitab0_{chunk}"):
            wait_bytes(recv_a.at[spot], a_recv_sem.at[chunk])
            wait_bytes(recv_b.at[spot], b_recv_sem.at[chunk])
        for tile in range(tiles):
            products = []
            for h in range(halves):
                at = chunk * piece + tile * halves + h
                product = lax.dot_general(
                    recv_a[at],
                    recv_b[at],
                    (((1,), (1,)), ((), ())),
                    preferred_element_type=jnp.float32,
                )
                products.append(product.reshape(row_part, halves, sub, product.shape[1]))
            for half in range(halves):
                packed = jnp.concatenate([product[:, half] for product in products], axis=1)
                send_x0[half, chunk, tile] = packed.astype(jnp.bfloat16)

    def multiply_second(chunk):
        spot = pl.ds(chunk * tiles, tiles)
        with jax.named_scope(f"waitab1_{chunk}"):
            wait_bytes(recv_ab.at[:, spot], ab_recv_sem.at[chunk])
        for tile in range(tiles):
            sides = []
            for which in range(2):
                got = recv_ab[which, chunk * tiles + tile].astype(jnp.float32)
                got = got.reshape(halves * row_part, halves, sub, got.shape[-1])
                sides.append(got)
            for h in range(halves):
                left, right = (
                    side[:, h]
                    .reshape(row_part * rows, side.shape[-1])
                    .astype(jnp.bfloat16)
                    for side in sides
                )
                send_x1[chunk * piece + tile * halves + h] = lax.dot_general(
                    left,
                    right,
                    (((0,), (0,)), ((), ())),
                    preferred_element_type=jnp.float32,
                ).astype(jnp.bfloat16)
        send_second_products(chunk, False)

    strip = min(hidden, 16)

    def strips(half):
        for at in range(0, hidden, strip):
            spot = pl.ds(at * sub, strip * sub)
            yield at, spot, stage_x[half, spot, :].reshape(strip, sub, cols)

    def fill(half, at, values):
        stage_x[half, pl.ds(at * sub, values.shape[0] * sub), :] = values.reshape(-1, cols)
        return jnp.sum(values, axis=0)

    def normalize_hidden(section, half, summed):
        center = summed * (1.0 / hidden)
        spread = jnp.zeros((sub, cols), jnp.float32)
        for _, _, values in strips(half):
            offset = values - center
            spread = spread + jnp.sum(offset * offset, axis=0)
        scale = lax.rsqrt(spread * (1.0 / hidden) + HIDDEN_EPSILON)
        for at, spot, values in strips(half):
            normed = (values - center) * scale * affine_t[section, 0, pl.ds(at, strip)]
            normed = normed + affine_t[section, 1, pl.ds(at, strip)]
            stage_x[half, spot, :] = normed.reshape(strip * sub, cols)

    def finish_first(half):
        with jax.named_scope(f"waitx0_{half}"):
            wait_bytes(recv_x0.at[half], x0_recv_sem.at[half])
        with jax.named_scope(f"finish0_{half}"):
            summed = jnp.zeros((sub, cols), jnp.float32)
            for chunk in range(chunks):
                for at in range(0, members * tiles, strip // halves):
                    height = min(strip // halves, members * tiles)
                    got = recv_x0[half, chunk, pl.ds(at, height)].astype(jnp.float32)
                    got = got.reshape(height * halves, sub, cols)
                    summed = summed + fill(half, chunk * wide + at * halves, got)
            normalize_hidden(0, half, summed)

            def finish(r):
                normed = stage_x[half, pl.ds(r - half * sub, hidden, stride=sub), :]
                projected = jnp.dot(
                    output_t[...],
                    normed.astype(jnp.bfloat16),
                    preferred_element_type=jnp.float32,
                )
                updated = pair_t[r] + gate[r] * (projected + lines_t[3])
                pair_t[r] = updated
                normed_ref[r] = normalize(updated, 0, PAIR_EPSILON, lines_t[4], lines_t[5])

            loop(half * sub, sub, finish)

    for chunk in range(chunks):
        with jax.named_scope(f"make0_{chunk}"):
            make_first(chunk)
    for at in later:
        loads[at].wait()
    with jax.named_scope("gates0"):
        prepare_lines()
        loop(0, rows, first_gates)
        prepare(1)
    for chunk in range(chunks):
        with jax.named_scope(f"mult0_{chunk}"):
            multiply_first(chunk)
            for half in range(halves):
                send_first_products(half, chunk, 1)

    lead = min(LEAD, chunks)

    def produce(half, chunk):
        with jax.named_scope(f"make1_{half}_{chunk}"):
            make_second(half, chunk)

    early_chunks = min(1, chunks) if halves > 1 else 0
    for half in range(halves):
        finish_first(half)
        if half < halves - 1:
            for chunk in range(early_chunks):
                produce(half, chunk)
    for chunk in range(lead):
        for half in range(halves):
            if not (half < halves - 1 and chunk < early_chunks):
                produce(half, chunk)
    for chunk in range(chunks):
        with jax.named_scope(f"mult1_{chunk}"):
            multiply_second(chunk)
        if chunk + lead < chunks:
            for half in range(halves):
                produce(half, chunk + lead)
        if chunk >= 1:
            send_second_products(chunk - 1, True)
    for chunk in range(chunks - 1, chunks):
        send_second_products(chunk, True)
    with jax.named_scope("gates1"):
        loop(0, rows, second_gates)
    summed = [jnp.zeros((sub, cols), jnp.float32) for _ in range(halves)]
    for chunk in range(chunks):
        with jax.named_scope(f"waitx1_{chunk}"):
            wait_bytes(recv_x1.at[:, pl.ds(chunk * wide, wide)], x1_recv_sem.at[chunk])
        for at in range(chunk * wide, (chunk + 1) * wide, min(strip, wide)):
            height = min(strip, wide)
            got = recv_x1[0, pl.ds(at, height)].astype(jnp.float32)
            for other in range(1, parts):
                got = got + recv_x1[other, pl.ds(at, height)].astype(jnp.float32)
            got = got.reshape(height, halves, sub, cols)
            for half in range(halves):
                summed[half] = summed[half] + fill(half, at, got[:, half])

    with jax.named_scope("finish1"):
        for half in range(halves):
            normalize_hidden(1, half, summed[half])

            def finish(r):
                normed = stage_x[half, pl.ds(r - half * sub, hidden, stride=sub), :]
                projected = lax.dot_general(
                    normed.astype(jnp.bfloat16),
                    held["output_weight"][1],
                    (((0,), (0,)), ((), ())),
                    preferred_element_type=jnp.float32,
                )
                out_ref[r] = held["pair"][r] + gate[r] * projected

            loop(half * sub, sub, finish)

    one = hidden - per_slot
    wait_bytes(send_ab0.at[0, pl.ds(0, one)], a_send_sem)
    wait_bytes(send_ab1.at[:, :, pl.ds(0, one // halves)], ab_send_sem)
    for distance in range(parts):
        amount = one if distance == 0 else hidden
        wait_bytes(send_ab0.at[1, pl.ds(0, amount)], b_send_sem.at[distance])
        wait_bytes(send_ab0.at[1, pl.ds(0, amount)], x1_send_sem.at[distance])
    wait_bytes(send_ab0.at[0, pl.ds(0, one)], x0_send_sem)


def local(row_total, col_total, pair_rep, residue_mask, *parameters):
    rows, cols, channels = pair_rep.shape
    hidden = parameters[2].shape[2] // 4
    parts = max(2, row_total * col_total // hidden)
    members = row_total * col_total // parts
    row_part = row_total // parts
    per_slot = hidden // members
    chunks = min(CHUNKS, per_slot)
    piece = per_slot // chunks
    halves = 2 if piece % 2 == 0 and rows % 16 == 0 else 1
    tiles = piece // halves
    sub = rows // halves
    wide = hidden // chunks
    total = row_total * rows
    part = total // parts
    sizes = (rows, cols, hidden, row_total, col_total, parts, chunks, halves)
    bf16, f32 = jnp.bfloat16, jnp.float32
    dma = pltpu.SemaphoreType.DMA
    arrays = (pair_rep, residue_mask.reshape(col_total, cols), *parameters)
    return pl.pallas_call(
        functools.partial(kernel, sizes),
        out_shape=pltpu.VMEM((rows, cols, channels), f32),
        in_specs=[pl.BlockSpec(memory_space=pltpu.HBM)] * (1 + len(arrays)),
        out_specs=pl.BlockSpec(memory_space=pltpu.VMEM),
        scratch_shapes=[pltpu.VMEM(array.shape, array.dtype) for array in arrays]
        + [
            pltpu.VMEM((2, 4 * hidden, channels), bf16),
            pltpu.VMEM((2, 4 * hidden, cols), f32),
            pltpu.VMEM((channels, channels), bf16),
            pltpu.VMEM((channels, hidden), bf16),
            pltpu.VMEM((6, channels, cols), f32),
            pltpu.VMEM((2, 2, hidden, sub, cols), f32),
            pltpu.VMEM((rows, channels, cols), bf16),
            pltpu.VMEM((2, wide * rows, cols), f32),
            pltpu.VMEM((halves, hidden * sub, cols), f32),
            pltpu.VMEM((rows, channels, cols), f32),
            pltpu.VMEM((rows, cols, channels), f32),
            pltpu.VMEM((2, hidden, rows, cols), bf16),
            pltpu.VMEM((2, halves, hidden // halves, rows, cols), bf16),
            pltpu.VMEM((per_slot, part, total), bf16),
            pltpu.VMEM((per_slot, total, total), bf16),
            pltpu.VMEM((2, per_slot // halves, halves, row_part, rows, total), bf16),
            pltpu.VMEM((halves, chunks, tiles, row_part, rows, total), bf16),
            pltpu.VMEM((per_slot, total, total), bf16),
            pltpu.VMEM((halves, chunks, members * tiles, rows, cols), bf16),
            pltpu.VMEM((parts, hidden, rows, cols), bf16),
            dma((len(arrays),)),
            dma(()),
            dma((chunks,)),
            dma((parts,)),
            dma((chunks,)),
            dma(()),
            dma((chunks,)),
            dma(()),
            dma((halves,)),
            dma((parts,)),
            dma((chunks,)),
            pltpu.SMEM(residue_mask.shape, residue_mask.dtype),
            dma(()),
        ],
        compiler_params=pltpu.CompilerParams(collective_id=0, has_side_effects=True),
    )(residue_mask, *arrays)


def solution(mesh):
    return jax.shard_map(
        functools.partial(local, mesh.shape["row"], mesh.shape["ch"]),
        mesh=mesh,
        in_specs=(P("row", "ch", None), P(), P(), P(), P(), P(), P(), P(), P(), P(), P(), P()),
        out_specs=P("row", "ch", None),
        check_vma=False,
    )
```
